256 devices in a mesh: seq: 64 (over z, y, core), batch: 4 (over x).
Axes of the slice: x: 4, y: 4, z: 8, core: 2. Of those that a mesh axis runs over, the one named last changes fastest.
Arguments:
- queries: bfloat16 [4, 32768, 16, 128], P('batch', 'seq'), may hold values from -5 to 5
- keys: bfloat16 [4, 32768, 16, 128], P('batch', 'seq'), may hold values from -5 to 5
- values: bfloat16 [4, 32768, 16, 128], P('batch', 'seq'), may hold values from -5 to 5
- keep_count: int32 [4, 16, 256], P('batch'), may hold values from 0 to 128
- query_map: bfloat16 [16, 128, 8], replicated, may hold values from -0.5 to 0.5
- key_map: bfloat16 [16, 128, 8], replicated, may hold values from -0.5 to 0.5
- cotangent: bfloat16 [4, 32768, 16, 128], P('batch', 'seq'), may hold values from -5 to 5
Outputs:
- attended: bfloat16 [4, 32768, 16, 128], P('batch', 'seq')
- grad_query_map: float32 [16, 128, 8], replicated
- grad_key_map: float32 [16, 128, 8], replicated
The draws below stay inside these ranges and needn't reach their ends.
All inputs are finite; a program needn't handle non-finite values.
Results may differ from the reference program's by a relative error of at most 0.0035.
Values may be sent and summed in bfloat16 or wider, within the bound.
No kernel may reach another device: no remote copies, remote signals or barrier semaphores. Data moves between devices by JAX's collectives and lax.ppermute only.
A program may use at most 128 MiB of HBM per device.

```python
import math
import jax
import jax.numpy as jnp
from jax import lax

HEADS = 16
DH = 128
RANK = 8
TILE = 128
WINDOW = 256
LEN = 32768
SEQS = 4
TILES = 256


def draw_queries(key, part):
    base = jax.random.truncated_normal(jax.random.fold_in(key, 1), -5.0, 5.0, (SEQS, LEN, HEADS, DH), jnp.float32)
    return base.astype(jnp.bfloat16)


def draw_keys(key, part):
    base = jax.random.truncated_normal(jax.random.fold_in(key, 2), -5.0, 5.0, (SEQS, LEN, HEADS, DH), jnp.float32)
    return base.astype(jnp.bfloat16)


def touch_ends(entries, key, least, top_value):
    longest = entries.shape.index(max(entries.shape))
    spots = []
    for shift in (0, 1):
        where = [jax.random.randint(jax.random.fold_in(key, axis), (), 0, length) for axis, length in enumerate(entries.shape)]
        where[longest] = (where[longest] + shift) % entries.shape[longest]
        spots.append(tuple(where))
    return entries.at[spots[0]].set(least).at[spots[1]].set(top_value)


def shard_levels(stream_key, dims, split, low, largest):
    factor_of, own = 1.0, jax.random.fold_in(stream_key, 6)
    for axis_at, parts in split:
        heights = jnp.exp(jax.random.uniform(jax.random.fold_in(own, axis_at), (parts,), jnp.float32, low / len(split), largest / len(split)))
        factor_of = factor_of * jnp.repeat(heights, dims[axis_at] // parts).reshape([-1 if axis == axis_at else 1 for axis in range(len(dims))])
    return factor_of


def centred(key, dims, scale, bound, split=(), kind=jnp.bfloat16):
    values = scale * jax.random.normal(key, dims, jnp.float32)
    if split:
        values = values * shard_levels(key, dims, split, -0.22, 0.18)
    return jnp.clip(values, -bound, bound).astype(kind)


def setup_inputs(seed: int = 0) -> dict:
    key_of = jax.random.split(jax.random.key(seed), 8)
    queries = draw_queries(jax.random.fold_in(key_of[7], 71), 0)
    keys = draw_keys(jax.random.fold_in(key_of[7], 71), 0)
    values = centred(key_of[2], (SEQS, LEN, HEADS, DH), 1.0, 5.0, ((0, 4), (1, 64)))
    keep_count = touch_ends(jax.random.randint(key_of[3], (SEQS, HEADS, TILES), 0, TILE + 1), jax.random.fold_in(key_of[3], 1), 0, TILE).astype(jnp.int32)
    query_map = centred(key_of[4], (HEADS, DH, RANK), DH ** -0.5, 0.5)
    key_map = centred(key_of[5], (HEADS, DH, RANK), DH ** -0.5, 0.5)
    cotangent = centred(key_of[6], (SEQS, LEN, HEADS, DH), 1.0, 5.0, ((0, 4), (1, 64)))
    return {"queries": queries, "keys": keys, "values": values, "keep_count": keep_count, "query_map": query_map, "key_map": key_map, "cotangent": cotangent}


HIGHEST = lax.Precision.HIGHEST
feature_shift = 1.5

def features(inputs, weights):
    pre_act = jnp.einsum('thd,hdr->thr', inputs.astype(jnp.float32), weights, precision=HIGHEST) - feature_shift
    return jax.nn.softplus(pre_act)

def shifted(array, offset):
    filler = jnp.zeros((offset,) + array.shape[1:], array.dtype)
    return jnp.concatenate([filler, array[:array.shape[0] - offset]], 0)

def exclusive(array):
    summed = jnp.cumsum(array, 0)
    return jnp.concatenate([jnp.zeros_like(array[:1]), summed[:-1]], 0)

def sparse_part(q_rows, k_rows, v_rows, kept):
    length, heads, width = q_rows.shape
    span = WINDOW // TILE
    scale = 1.0 / math.sqrt(width)
    filler = jnp.zeros((WINDOW, heads, width), k_rows.dtype)
    k_padded = jnp.concatenate([filler, k_rows], 0)
    v_padded = jnp.concatenate([filler, v_rows], 0)
    kept_padded = jnp.concatenate([jnp.zeros((WINDOW, heads), bool), kept], 0)

    def one_block(block):
        start = (block * WINDOW).astype(jnp.int32)
        q_block = lax.dynamic_slice_in_dim(q_rows, start, WINDOW, 0)
        k_block = lax.dynamic_slice_in_dim(k_padded, start, 2 * WINDOW, 0)
        v_block = lax.dynamic_slice_in_dim(v_padded, start, 2 * WINDOW, 0)
        kept_block = lax.dynamic_slice_in_dim(kept_padded, start, 2 * WINDOW, 0)
        q_pos = start + jnp.arange(WINDOW, dtype=jnp.int32)
        k_pos = start - WINDOW + jnp.arange(2 * WINDOW, dtype=jnp.int32)
        scores = jnp.einsum('thd,phd->htp', q_block.astype(jnp.float32), k_block.astype(jnp.float32)) * scale
        tile_gap = q_pos[:, None] // TILE - k_pos[None, :] // TILE
        causal = (k_pos[None, :] <= q_pos[:, None]) & (k_pos[None, :] >= 0) & (tile_gap < span)
        live_pairs = causal[None] & ((tile_gap == 0)[None] | kept_block.T[:, None, :])
        row_max = lax.optimization_barrier(jnp.max(jnp.where(live_pairs, scores, -jnp.inf), -1))
        weights = jnp.where(live_pairs, jnp.exp(scores - row_max[..., None]), 0.0)
        denom = lax.optimization_barrier(jnp.sum(weights, -1))
        numer = jnp.einsum('htp,phd->thd', weights.astype(jnp.bfloat16).astype(jnp.float32), v_block.astype(jnp.float32))
        return (numer, denom.T, row_max.T)
    numer, denom, row_max = lax.map(one_block, jnp.arange(length // WINDOW, dtype=jnp.int32))
    return (numer.reshape(length, heads, width), denom.reshape(length, heads), row_max.reshape(length, heads))

def reference(queries, keys, values, keep_count, query_map, key_map, cotangent):
    query_weights = query_map.astype(jnp.float32)
    key_weights = key_map.astype(jnp.float32)
    span = WINDOW // TILE

    def one_sequence(inputs):
        q_rows, k_rows, v_rows, counts, cot_rows = inputs
        length, heads, width = q_rows.shape
        tiles = length // TILE
        within = jnp.arange(length, dtype=jnp.int32) % TILE
        kept = within[:, None] < jnp.repeat(counts, TILE, axis=1).T
        numer, denom, row_max = sparse_part(q_rows, k_rows, v_rows, kept)
        decay = jnp.exp(-row_max)
        v_tiles = v_rows.astype(jnp.float32).reshape(tiles, TILE, heads, width)
        evicted = (1 - kept.astype(jnp.float32)).reshape(tiles, TILE, heads, 1)

        def linear(q_weights, k_weights):
            feat_q = features(q_rows, q_weights).reshape(tiles, TILE, heads, RANK)
            feat_k = features(k_rows, k_weights).reshape(tiles, TILE, heads, RANK)
            all_state = jnp.einsum('nthr,nthd->nhrd', feat_k, v_tiles, precision=HIGHEST)
            all_norm = lax.optimization_barrier(jnp.sum(feat_k, 1))
            ev_feat = feat_k * evicted
            ev_state = jnp.einsum('nthr,nthd->nhrd', ev_feat, v_tiles, precision=HIGHEST)
            ev_norm = lax.optimization_barrier(jnp.sum(ev_feat, 1))
            state = shifted(exclusive(all_state), span - 1)
            norm = shifted(exclusive(all_norm), span - 1)
            for offset in range(1, span):
                state = state + shifted(ev_state, offset)
                norm = norm + shifted(ev_norm, offset)
            kernel_num = jnp.einsum('nthr,nhrd->nthd', feat_q, state, precision=HIGHEST).reshape(length, heads, width)
            kernel_den = jnp.einsum('nthr,nhr->nth', feat_q, norm, precision=HIGHEST).reshape(length, heads)
            return (numer + decay[..., None] * kernel_num) / (denom + decay * kernel_den)[..., None]
        out, pull_back = jax.vjp(linear, query_weights, key_weights)
        grad_q, grad_k = pull_back(cot_rows.astype(jnp.float32))
        return (out.astype(jnp.bfloat16), grad_q, grad_k)
    attended, grad_q, grad_k = lax.map(one_sequence, (queries, keys, values, keep_count, cotangent))
    return (attended, lax.optimization_barrier(jnp.sum(grad_q, 0)), lax.optimization_barrier(jnp.sum(grad_k, 0)))
```

```python
import functools
import math

import jax
import jax.numpy as jnp
from jax import lax
from jax.experimental import pallas as pl
from jax.experimental.pallas import tpu as pltpu
from jax.sharding import Mesh
from jax.sharding import PartitionSpec as P

TILE = 128
HEADS = 16
RANK = 8
DH = 128
ROWS = HEADS * RANK
SEQ = ("z", "y", "core")
ALL = ("z", "y", "core", "batch")
SHIFT = 1.5
SCALE = 1.0 / math.sqrt(DH)
SCALE_LOG2 = SCALE * math.log2(math.e)
NEG = -1e30
F32 = jnp.float32
BF16 = jnp.bfloat16
NT = (((1,), (1,)), ((), ()))
TN = (((0,), (0,)), ((), ()))
NN = (((1,), (0,)), ((), ()))


def dot(a, b, dims=NN):
    return lax.dot_general(a, b, dims, preferred_element_type=F32)


def halves(x):
    hi = x.astype(BF16)
    return hi, (x - hi.astype(F32)).astype(BF16)


def stacked(x):
    hi = x.astype(BF16).astype(F32)
    return jnp.concatenate([hi, x - hi], 0).astype(BF16)


def folded(x):
    return x[:RANK] + x[RANK : 2 * RANK]


def row_sums(x):
    ones = jnp.ones((8, 128), BF16)
    hi, lo = halves(x)
    return dot(ones, hi, NT) + dot(ones, lo, NT)


def softplus_sigmoid(pre):
    e = jnp.exp(-jnp.abs(pre))
    value = jnp.maximum(pre, 0.0) + jnp.log1p(e)
    inv = 1.0 / (1.0 + e)
    return value, jnp.where(pre >= 0, inv, e * inv)


def per_head_sum(x):
    x = x.reshape(HEADS, RANK, TILE)
    x = jnp.broadcast_to(jnp.sum(x, 1, keepdims=True), x.shape)
    return x.reshape(ROWS, TILE)


def head_rows(h):
    return pl.ds(h * RANK, RANK)


def lane(x, k):
    at = lax.broadcasted_iota(jnp.int32, x.shape, 1) == k
    return jnp.sum(jnp.where(at, x, 0.0), 1, keepdims=True)


def keys_kernel(idx_ref, cnt_ref, k_ref, v_ref, kmap_ref, kh_ref, vh_ref, local_ref,
                sig_ref, evict_ref, nloc_ref, msg_ref, kscr, vscr, pre, all_acc, nacc, feats):
    n = pl.program_id(0)

    @pl.when(n == 0)
    def _():
        all_acc[...] = jnp.zeros_like(all_acc)
        nacc[...] = jnp.zeros_like(nacc)

    kscr[...] = k_ref[0].reshape(TILE * HEADS, DH).astype(F32)
    vscr[...] = v_ref[0].reshape(TILE * HEADS, DH).astype(F32)
    lanes = lax.broadcasted_iota(jnp.int32, (RANK, TILE), 1)
    for h in range(HEADS):
        kh = kscr[pl.ds(h, TILE, stride=HEADS), :].astype(BF16)
        kh_ref[h] = kh
        vh_ref[h] = vscr[pl.ds(h, TILE, stride=HEADS), :].astype(BF16)
        pre[head_rows(h), :] = dot(kmap_ref[h], kh, NT)
        count = cnt_ref[h, idx_ref[0] * 4 + n]
        evict_ref[0, head_rows(h), :] = (lanes >= count).astype(F32)
    feat, sig = softplus_sigmoid(pre[...] - SHIFT)
    sig_ref[0] = sig
    ev = feat * evict_ref[0]
    feats[0] = feat
    feats[1] = ev
    for h in range(HEADS):
        lhs = jnp.concatenate(
            [stacked(feats[0, head_rows(h), :]), stacked(feats[1, head_rows(h), :])], 0
        )
        res = dot(lhs, vh_ref[h])
        before = all_acc[head_rows(h), :]
        local_ref[0, head_rows(h), :] = before_last(before, folded(res[2 * RANK :]), n)
        all_acc[head_rows(h), :] = before + folded(res)
    all_norm = jnp.sum(feat, 1, keepdims=True)
    ev_norm = jnp.sum(ev, 1, keepdims=True)
    nloc_ref[0] = jnp.broadcast_to(ev_norm, (ROWS, TILE)) + nacc[...]
    nacc[...] += jnp.broadcast_to(all_norm, (ROWS, TILE))

    @pl.when(n == 3)
    def _():
        row = row_sums(nacc[...] * (1.0 / 128.0))
        for s in range(64):
            msg_ref[s, 0:2, :] = all_acc[2 * s : 2 * s + 2, :]
            msg_ref[s, 2:4, :] = row[0:2]


def before_last(before, ev, n):
    return before + ev


def attend_kernel(idx_ref, cnt_ref, q_ref, c_ref, kh_ref, vh_ref, hk_ref, hv_ref, qmap_ref,
                  kmap_ref, nloc_ref, got_ref, qh_ref, ch_ref, numer_ref, stats_ref, dst_ref,
                  halo_k_ref, halo_v_ref, halo_ref, msg_ref,
                  qscr, cscr, pk, pv, pre, mx, den, cn, norm, cf, dacc):
    t = pl.program_id(0)
    index = idx_ref[0]
    lanes = lax.broadcasted_iota(jnp.int32, (RANK, TILE), 1)

    @pl.when(t == 0)
    def _():
        dacc[...] = jnp.zeros_like(dacc)
        run = jnp.zeros((2, 128), F32)
        nrun = jnp.zeros((1, 128), F32)
        for s in range(64):
            msg_ref[s, 0:2, :] = run
            run = run + got_ref[s, 0:2, :]
            nrun = nrun + jnp.where(s < index, got_ref[s, 2:3, :], 0.0)
        norm[...] = jnp.broadcast_to(nrun, (128, 128)).T
        qscr[...] = hk_ref[...].reshape(TILE * HEADS, DH).astype(F32)
        cscr[...] = hv_ref[...].reshape(TILE * HEADS, DH).astype(F32)
        for h in range(HEADS):
            kh = qscr[pl.ds(h, TILE, stride=HEADS), :].astype(BF16)
            vh = cscr[pl.ds(h, TILE, stride=HEADS), :].astype(BF16)
            pk[h] = kh
            pv[h] = vh
            halo_k_ref[h] = kh
            halo_v_ref[h] = vh
            pre[head_rows(h), :] = dot(kmap_ref[h], kh, NT)
            count = jnp.where(index > 0, cnt_ref[h, jnp.maximum(index * 4 - 1, 0)], 0)
            halo_ref[1, head_rows(h), :] = (lanes < count).astype(F32)
        feat, sig = softplus_sigmoid(pre[...] - SHIFT)
        feat = feat * halo_ref[1]
        halo_ref[1] = halo_ref[1] * sig
        cf[...] = feat
        for h in range(HEADS):
            halo_ref[0, head_rows(h), :] = folded(dot(stacked(cf[head_rows(h), :]), pv[h]))
        kept_norm = jnp.sum(feat, 1, keepdims=True)
        stats_ref[0, 5] = norm[...] - kept_norm

    @pl.when(t > 0)
    def _():
        stats_ref[0, 5] = norm[...] + nloc_ref[0]

    qscr[...] = q_ref[0].reshape(TILE * HEADS, DH).astype(F32)
    cscr[...] = c_ref[0].reshape(TILE * HEADS, DH).astype(F32)
    rows = lax.broadcasted_iota(jnp.int32, (TILE, TILE), 0)
    cols = lax.broadcasted_iota(jnp.int32, (TILE, TILE), 1)
    causal = rows <= cols
    for h in range(HEADS):
        qh = qscr[pl.ds(h, TILE, stride=HEADS), :].astype(BF16)
        ch = cscr[pl.ds(h, TILE, stride=HEADS), :].astype(BF16)
        qh_ref[h] = qh
        ch_ref[h] = ch
        pre[head_rows(h), :] = dot(qmap_ref[h], qh, NT)
        before = index * 4 + t - 1
        count = jnp.where(before >= 0, cnt_ref[h, jnp.maximum(before, 0)], 0)
        vp, vo = pv[h], vh_ref[h]
        s_prev = jnp.where(rows < count, dot(pk[h], qh, NT), NEG)
        s_own = jnp.where(causal, dot(kh_ref[h], qh, NT), NEG)
        top = jnp.max(jnp.maximum(s_prev, s_own), 0, keepdims=True)
        w_prev = jnp.exp2((s_prev - top) * SCALE_LOG2)
        w_own = jnp.exp2((s_own - top) * SCALE_LOG2)
        sums = jnp.sum(w_prev + w_own, 0, keepdims=True)
        b_prev, b_own = w_prev.astype(BF16), w_own.astype(BF16)
        numer_ref[h] = dot(b_prev, vp, TN) + dot(b_own, vo, TN)
        against = b_prev.astype(F32) * dot(vp, ch, NT) + b_own.astype(F32) * dot(vo, ch, NT)
        mx[head_rows(h), :] = jnp.broadcast_to(top, (RANK, TILE))
        den[head_rows(h), :] = jnp.broadcast_to(sums, (RANK, TILE))
        cn[head_rows(h), :] = jnp.broadcast_to(jnp.sum(against, 0, keepdims=True), (RANK, TILE))
    pk[...] = kh_ref[...]
    pv[...] = vh_ref[...]
    feat, sig = softplus_sigmoid(pre[...] - SHIFT)
    decay = jnp.exp(-(mx[...] * SCALE))
    total = den[...] + decay * per_head_sum(feat * stats_ref[0, 5])
    rinv = 1.0 / total
    coef = decay * rinv
    stats_ref[0, 0] = feat
    stats_ref[0, 1] = sig
    stats_ref[0, 2] = coef
    stats_ref[0, 3] = rinv
    stats_ref[0, 4] = cn[...] * rinv
    cf[...] = feat * coef
    for h in range(HEADS):
        d = folded(dot(stacked(cf[head_rows(h), :]), ch_ref[h]))
        dst_ref[0, head_rows(h), :] = d
        dacc[head_rows(h), :] += d

    @pl.when(t == 3)
    def _():
        for s in range(64):
            msg_ref[s, 2:4, :] = dacc[2 * s : 2 * s + 2, :]


def output_kernel(numer_ref, qh_ref, ch_ref, stats_ref, local_ref, halo_ref, got_ref, out_ref,
                  gq_ref, dn_ref, msg_ref, far, state, oscr, grad, cf, drow):
    t = pl.program_id(0)

    @pl.when(t == 0)
    def _():
        gq_ref[...] = jnp.zeros_like(gq_ref)
        drow[...] = jnp.zeros_like(drow)
        for s in range(64):
            far[2 * s : 2 * s + 2, :] = got_ref[s, 0:2, :]
        run = jnp.zeros((2, 128), F32)
        for s in reversed(range(64)):
            msg_ref[s, 0:2, :] = run
            run = run + got_ref[s, 2:4, :]
        state[...] = far[...] - halo_ref[0]

    @pl.when(t > 0)
    def _():
        state[...] = far[...] + local_ref[0]

    feat, sig, coef, rinv, cnr, norm = (stats_ref[0, i] for i in range(6))
    cf[...] = feat * coef
    sub = lax.broadcasted_iota(jnp.int32, (RANK, TILE), 0)
    ones = jnp.ones((RANK, DH), F32)
    zeros = jnp.zeros((RANK, DH), F32)
    for h in range(HEADS):
        s = state[head_rows(h), :]
        s_hi = s.astype(BF16).astype(F32)
        s_lo = s - s_hi
        grad[head_rows(h), :] = folded(
            dot(jnp.concatenate([s_hi, s_lo], 0).astype(BF16), ch_ref[h], NT)
        )
        c = cf[head_rows(h), :]
        c_hi = c.astype(BF16).astype(F32)
        r = stats_ref[0, 3, head_rows(h), :]
        r_hi = r.astype(BF16).astype(F32)
        r_mid = (r - r_hi).astype(BF16).astype(F32)
        pieces = jnp.where(sub == 0, r_hi, jnp.where(sub == 1, r_mid, jnp.where(sub == 2, r - r_hi - r_mid, 0.0)))
        lhs = jnp.concatenate([c_hi, c - c_hi, c_hi, pieces], 0).astype(BF16)
        rhs = jnp.concatenate(
            [
                jnp.concatenate([s_hi, s_hi, s_lo, zeros], 0),
                jnp.concatenate([zeros, zeros, zeros, ones], 0),
            ],
            1,
        ).astype(BF16)
        both = dot(lhs, rhs, TN)
        oscr[pl.ds(h, TILE, stride=HEADS), :] = numer_ref[h] * both[:, DH:] + both[:, :DH]
    out_ref[0] = oscr[...].astype(BF16).reshape(TILE, HEADS, DH)
    g = grad[...]
    along = cnr + per_head_sum(cf[...] * g)
    grad[...] = coef * (g - along * norm) * sig
    for h in range(HEADS):
        gq_ref[head_rows(h), :] += folded(dot(stacked(grad[head_rows(h), :]), qh_ref[h]))
    dn = -(cf[...] * along)
    dn_ref[0] = jnp.broadcast_to(jnp.sum(dn, 1, keepdims=True), (ROWS, TILE))
    drow[...] += row_sums(dn)

    @pl.when(t == 3)
    def _():
        for s in range(64):
            msg_ref[s, 2:4, :] = drow[0:2, :]


def key_grad_kernel(idx_ref, kh_ref, vh_ref, sig_ref, evict_ref, dst_ref, dn_ref, halo_k_ref,
                    halo_v_ref, halo_ref, got_ref, gq_ref, out_ref, acc, nacc, grad, ev):
    i = pl.program_id(0)
    n = 3 - i
    index = idx_ref[0]

    @pl.when(i == 0)
    def _():
        out_ref[:ROWS, :] = gq_ref[...]
        nrun = jnp.zeros((1, 128), F32)
        for s in range(64):
            acc[2 * s : 2 * s + 2, :] = got_ref[s, 0:2, :]
            nrun = nrun + jnp.where(s > index, got_ref[s, 2:3, :], 0.0)
        nacc[...] = jnp.broadcast_to(nrun, (128, 128)).T
        for h in range(HEADS):
            grad[head_rows(h), :] = folded(
                dot(stacked(dst_ref[0, head_rows(h), :]), halo_v_ref[h], NT)
            )
        grad[...] = -(grad[...] + dn_ref[0]) * halo_ref[1]
        for h in range(HEADS):
            out_ref[pl.ds(ROWS + h * RANK, RANK), :] = folded(
                dot(stacked(grad[head_rows(h), :]), halo_k_ref[h])
            )

    @pl.when(i >= 2)
    def _():
        acc[...] += dst_ref[jnp.minimum(n + 2, 3)]
        nacc[...] += dn_ref[jnp.minimum(n + 2, 3)]

    after = jnp.minimum(n + 1, 3)
    live = (n < 3).astype(F32)
    for h in range(HEADS):
        lhs = jnp.concatenate(
            [stacked(acc[head_rows(h), :]), stacked(dst_ref[after, head_rows(h), :] * live)], 0
        )
        res = dot(lhs, vh_ref[h], NT)
        grad[head_rows(h), :] = folded(res)
        ev[head_rows(h), :] = folded(res[2 * RANK :])
    near = ev[...] + dn_ref[after] * live
    grad[...] = (grad[...] + nacc[...] + evict_ref[0] * near) * sig_ref[0]
    for h in range(HEADS):
        out_ref[pl.ds(ROWS + h * RANK, RANK), :] += folded(
            dot(stacked(grad[head_rows(h), :]), kh_ref[h])
        )


def total_kernel(x_ref, o_ref):
    o_ref[...] = jnp.broadcast_to(jnp.sum(x_ref[...], 0, keepdims=True), o_ref.shape)


def sds(shape, dtype=F32):
    return jax.ShapeDtypeStruct(shape, dtype)


def whole(shape):
    return pl.BlockSpec(shape, lambda *_: (0,) * len(shape))


SMEM = pl.BlockSpec(memory_space=pltpu.SMEM)
MAPS = whole((HEADS, RANK, DH))
MSG = whole((64, 4, 128))
NAT = pl.BlockSpec((1, TILE, HEADS, DH), lambda t: (0, t, 0, 0))
BYHEAD = pl.BlockSpec((HEADS, TILE, DH), lambda t: (0, t, 0))
PART = pl.BlockSpec((1, ROWS, TILE), lambda t: (t, 0, 0))
PREV = pl.BlockSpec((1, ROWS, TILE), lambda t: (jnp.maximum(t - 1, 0), 0, 0))
STATS = pl.BlockSpec((1, 6, ROWS, TILE), lambda t: (t, 0, 0, 0))
HALO = whole((HEADS, TILE, DH))
BIG = sds((HEADS, 4 * TILE, DH), BF16)
PARTS = sds((4, ROWS, TILE))
SQ = pltpu.VMEM((ROWS, TILE), F32)
FLAT = pltpu.VMEM((TILE * HEADS, DH), F32)
MSG_T = sds((64, 4, 128))


def exchanged(x, axes):
    return lax.all_to_all(x, axes, split_axis=0, concat_axis=0, tiled=True)


def call(kernel, name, grid, in_specs, out_specs, out_shape, scratch):
    return pl.pallas_call(
        kernel,
        grid=(grid,),
        in_specs=in_specs,
        out_specs=out_specs,
        out_shape=out_shape,
        scratch_shapes=scratch,
        name=name,
        compiler_params=pltpu.CompilerParams(
            dimension_semantics=("arbitrary",), vmem_limit_bytes=40 * 2**20
        ),
    )


def body(queries, keys, values, keep_count, query_map, key_map, cotangent):
    count = lax.axis_size(SEQ)
    steps = [(i, i + 1) for i in range(count - 1)]
    halo_k = lax.ppermute(keys[0, 3 * TILE :], SEQ, steps)
    halo_v = lax.ppermute(values[0, 3 * TILE :], SEQ, steps)
    index = lax.axis_index(SEQ).astype(jnp.int32).reshape(1)
    counts = keep_count[0]
    qmap = query_map.transpose(0, 2, 1)
    kmap = key_map.transpose(0, 2, 1)

    kh, vh, local, sig_k, evict, nloc, msg = call(
        keys_kernel, "keys", 4,
        [SMEM, SMEM, NAT, NAT, MAPS],
        [BYHEAD, BYHEAD, PART, PART, PART, PART, MSG],
        [BIG, BIG, PARTS, PARTS, PARTS, PARTS, MSG_T],
        [FLAT, FLAT, SQ, SQ, SQ, pltpu.VMEM((2, ROWS, TILE), F32)],
    )(index, counts, keys, values, kmap)

    got = exchanged(msg, SEQ)

    qh, ch, numer, stats, dst, hk, hv, halo, msg = call(
        attend_kernel, "attend", 4,
        [SMEM, SMEM, NAT, NAT, BYHEAD, BYHEAD, HALO_NAT, HALO_NAT, MAPS, MAPS, PREV, MSG],
        [BYHEAD, BYHEAD, BYHEAD, STATS, PART, HALO, HALO, whole((2, ROWS, TILE)), MSG],
        [BIG, BIG, sds((HEADS, 4 * TILE, DH)), sds((4, 6, ROWS, TILE)), PARTS,
         sds((HEADS, TILE, DH), BF16), sds((HEADS, TILE, DH), BF16), sds((2, ROWS, TILE)), MSG_T],
        [FLAT, FLAT, pltpu.VMEM((HEADS, TILE, DH), BF16), pltpu.VMEM((HEADS, TILE, DH), BF16),
         SQ, SQ, SQ, SQ, SQ, SQ, SQ],
    )(index, counts, queries, cotangent, kh, vh, halo_k, halo_v, qmap, kmap, nloc, got)

    got = exchanged(msg, SEQ)

    out, gq, dn, msg = call(
        output_kernel, "output", 4,
        [BYHEAD, BYHEAD, BYHEAD, STATS, PREV, whole((2, ROWS, TILE)), MSG],
        [NAT, whole((ROWS, TILE)), PART, MSG],
        [sds((1, 4 * TILE, HEADS, DH), BF16), sds((ROWS, TILE)), PARTS, MSG_T],
        [SQ, SQ, FLAT, SQ, SQ, pltpu.VMEM((8, 128), F32)],
    )(numer, qh, ch, stats, local, halo, got)

    got = exchanged(msg, SEQ)

    back = lambda t: (0, 3 - t, 0)
    part = lambda t: (3 - t, 0, 0)
    grads = call(
        key_grad_kernel, "key_grad", 4,
        [SMEM, pl.BlockSpec((HEADS, TILE, DH), back), pl.BlockSpec((HEADS, TILE, DH), back),
         pl.BlockSpec((1, ROWS, TILE), part), pl.BlockSpec((1, ROWS, TILE), part),
         whole((4, ROWS, TILE)), whole((4, ROWS, TILE)), HALO, HALO, whole((2, ROWS, TILE)), MSG,
         whole((ROWS, TILE))],
        whole((2 * ROWS, TILE)),
        sds((2 * ROWS, TILE)),
        [SQ, SQ, SQ, SQ],
    )(index, kh, vh, sig_k, evict, dst, dn, hk, hv, halo, got, gq)

    arrived = exchanged(grads.reshape(256, 1, 128), ALL).reshape(256, 128)
    copies = pl.pallas_call(total_kernel, out_shape=sds((256, 128)), name="total")(arrived)
    whole_sum = exchanged(copies.reshape(256, 1, 128), ALL).reshape(2, HEADS, RANK, DH)
    grad_q, grad_k = whole_sum.transpose(0, 1, 3, 2)
    return out, grad_q, grad_k


HALO_NAT = whole((TILE, HEADS, DH))


def solution(mesh):
    torus = Mesh(mesh.devices.reshape(8, 4, 2, mesh.shape["batch"]), ALL)
    rows = P("batch", SEQ, None, None)
    in_specs = (rows, rows, rows, P("batch", None, None), P(), P(), rows)
    return jax.shard_map(
        body, mesh=torus, in_specs=in_specs, out_specs=(rows, P(), P()), check_vma=False
    )
```

```python
import math

import jax
import jax.numpy as jnp
from jax import lax
from jax.experimental import pallas as pl
from jax.experimental.pallas import tpu as pltpu
from jax.sharding import Mesh
from jax.sharding import PartitionSpec as P

TILE = 128
HEADS = 16
RANK = 8
DH = 128
ROWS = HEADS * RANK
SEQ = ("z", "y", "core")
ALL = ("z", "y", "core", "batch")
SHIFT = 1.5
SCALE = 1.0 / math.sqrt(DH)
SCALE_LOG2 = SCALE * math.log2(math.e)
NEG = -1e30
VMEM = 67_043_328
F32 = jnp.float32
BF16 = jnp.bfloat16
NN = (((1,), (0,)), ((), ()))
NT = (((1,), (1,)), ((), ()))
TN = (((0,), (0,)), ((), ()))


def dot(a, b, dims=NN):
    return lax.dot_general(a, b, dims, preferred_element_type=F32)


def halves(x):
    hi = x.astype(BF16)
    return hi, (x - hi.astype(F32)).astype(BF16)


def stacked(*parts):
    rows = []
    for x in parts:
        hi = x.astype(BF16).astype(F32)
        rows += [hi, x - hi]
    return jnp.concatenate(rows, 0).astype(BF16)


def folded(x, at=0):
    return x[at : at + RANK] + x[at + RANK : at + 2 * RANK]


def row_sums(x):
    ones = jnp.ones((8, 128), BF16)
    hi, lo = halves(x)
    return dot(ones, hi, NT) + dot(ones, lo, NT)


def softplus_sigmoid(pre):
    e = jnp.exp(-jnp.abs(pre))
    value = jnp.maximum(pre, 0.0) + jnp.log1p(e)
    inv = 1.0 / (1.0 + e)
    return value, jnp.where(pre >= 0, inv, e * inv)


def per_head_sum(x):
    x = x.reshape(HEADS, RANK, TILE)
    x = jnp.broadcast_to(jnp.sum(x, 1, keepdims=True), x.shape)
    return x.reshape(ROWS, TILE)


def of(h):
    return pl.ds(h * RANK, RANK)


def lane_sums(x):
    return jnp.broadcast_to(jnp.sum(x, 1, keepdims=True), (ROWS, TILE))


def keys_kernel(idx_ref, cnt_ref, k_ref, v_ref, kmap_ref, kh_ref, vh_ref, halo_ref, local_ref,
                sig_ref, evict_ref, nloc_ref, msg_ref, pre, evict, st_all, st_ev, all_acc, nacc,
                feats, msg):
    n = pl.program_id(0)

    @pl.when(n == 0)
    def _():
        all_acc[...] = jnp.zeros_like(all_acc)
        nacc[...] = jnp.zeros_like(nacc)

    kh_ref[...] = jnp.swapaxes(k_ref[0], 0, 1)
    vh_ref[...] = jnp.swapaxes(v_ref[0], 0, 1)
    lanes = lax.broadcasted_iota(jnp.int32, (RANK, TILE), 1)
    for h in range(HEADS):
        pre[of(h), :] = dot(kmap_ref[h], kh_ref[h], NT)
        count = cnt_ref[h, idx_ref[0] * 4 + n]
        evict[of(h), :] = (lanes >= count).astype(F32)
    feat, sig = softplus_sigmoid(pre[...] - SHIFT)
    ev = feat * evict[...]
    feats[0] = feat
    feats[1] = ev
    for h in range(HEADS):
        res = dot(stacked(feats[0, of(h), :], feats[1, of(h), :]), vh_ref[h])
        st_all[of(h), :] = folded(res)
        st_ev[of(h), :] = folded(res, 2 * RANK)
    evict_ref[0] = evict[...]
    sig_ref[0] = sig
    local_ref[0] = all_acc[...] + st_ev[...]
    all_acc[...] += st_all[...]
    nloc_ref[0] = lane_sums(ev) + nacc[...]
    nacc[...] += lane_sums(feat)

    @pl.when(n == 3)
    def _():
        halo_ref[0] = kh_ref[...]
        halo_ref[1] = vh_ref[...]
        row = row_sums(nacc[...] * (1.0 / 128.0))
        for s in range(64):
            msg[s, 0:2, :] = all_acc[2 * s : 2 * s + 2, :]
            msg[s, 2:4, :] = row[0:2]
        msg_ref[...] = msg[...]


def attention(kp_ref, ko_ref, vp_ref, vo_ref, qmap_ref, count_of, qs, cs, raw_ref, numer_ref,
              scores, weights, vv, pre, mx, den, cn):
    zeros = jnp.zeros((RANK, DH), F32)
    for h in range(HEADS):
        vv[h, 0:TILE, :] = vp_ref[h]
        vv[h, TILE:, :] = vo_ref[h]
        top = jnp.concatenate([qmap_ref[h].astype(F32), zeros], 0).astype(BF16)
        res = dot(jnp.concatenate([top, kp_ref[h], ko_ref[h]], 0), qs[h], NT)
        pre[of(h), :] = res[:RANK]
        scores[h] = res[2 * RANK :]
    rows = lax.broadcasted_iota(jnp.int32, (TILE, TILE), 0)
    cols = lax.broadcasted_iota(jnp.int32, (TILE, TILE), 1)
    causal = rows <= cols
    for h in range(HEADS):
        s_prev = jnp.where(rows < count_of(h), scores[h, 0:TILE, :], NEG)
        s_own = jnp.where(causal, scores[h, TILE:, :], NEG)
        top = jnp.max(jnp.maximum(s_prev, s_own), 0, keepdims=True)
        w_prev = jnp.exp2((s_prev - top) * SCALE_LOG2)
        w_own = jnp.exp2((s_own - top) * SCALE_LOG2)
        weights[h, 0:TILE, :] = w_prev.astype(BF16)
        weights[h, TILE:, :] = w_own.astype(BF16)
        sums = jnp.sum(w_prev + w_own, 0, keepdims=True)
        mx[of(h), :] = jnp.broadcast_to(top, (RANK, TILE))
        den[of(h), :] = jnp.broadcast_to(sums, (RANK, TILE))
    for h in range(HEADS):
        w = weights[h]
        against = w.astype(F32) * dot(vv[h], cs[h], NT)
        cn[of(h), :] = jnp.broadcast_to(jnp.sum(against, 0, keepdims=True), (RANK, TILE))
        numer_ref[h] = dot(w, vv[h], TN)
    feat, sig = softplus_sigmoid(pre[...] - SHIFT)
    raw_ref[0, 0] = feat
    raw_ref[0, 1] = sig
    raw_ref[0, 2] = jnp.exp(-(mx[...] * SCALE))
    raw_ref[0, 3] = den[...]
    raw_ref[0, 4] = cn[...]


def near_kernel(idx_ref, cnt_ref, q_ref, c_ref, kp_ref, ko_ref, vp_ref, vo_ref, qmap_ref, qh_ref,
                ch_ref, numer_ref, raw_ref, qs, cs, *scratch):
    t = pl.program_id(0)
    qs[...] = jnp.swapaxes(q_ref[0], 0, 1)
    cs[...] = jnp.swapaxes(c_ref[0], 0, 1)

    @pl.when(t > 0)
    def _():
        before = idx_ref[0] * 4 + jnp.maximum(t - 1, 0)
        attention(kp_ref, ko_ref, vp_ref, vo_ref, qmap_ref, lambda h: cnt_ref[h, before], qs, cs,
                  raw_ref, numer_ref, *scratch)

    qh_ref[...] = qs[...]
    ch_ref[...] = cs[...]


def first_kernel(idx_ref, cnt_ref, qh_ref, ch_ref, halo_in, ko_ref, vo_ref, qmap_ref, kmap_ref,
                 numer_any, raw_any, numer_ref, raw_ref, halo_ref, nhalo_ref, qs, cs, kept, feats,
                 *scratch):
    del numer_any, raw_any
    index = idx_ref[0]
    before = jnp.maximum(index * 4 - 1, 0)
    pre = scratch[3]
    lanes = lax.broadcasted_iota(jnp.int32, (RANK, TILE), 1)
    counts = [jnp.where(index > 0, cnt_ref[h, before], 0) for h in range(HEADS)]
    qs[...] = qh_ref[...]
    cs[...] = ch_ref[...]
    for h in range(HEADS):
        pre[of(h), :] = dot(kmap_ref[h], halo_in[0, h], NT)
        kept[of(h), :] = (lanes < counts[h]).astype(F32)
    feat, sig = softplus_sigmoid(pre[...] - SHIFT)
    feat = feat * kept[...]
    feats[...] = feat
    for h in range(HEADS):
        feats[of(h), :] = folded(dot(stacked(feats[of(h), :]), halo_in[1, h]))
    halo_ref[0] = feats[...]
    halo_ref[1] = kept[...] * sig
    nhalo_ref[...] = lane_sums(feat)
    attention(halo_in.at[0], ko_ref, halo_in.at[1], vo_ref, qmap_ref, lambda h: counts[h], qs, cs,
              raw_ref, numer_ref, *scratch)


def total_kernel(idx_ref, raw_ref, ch_ref, nloc_ref, nhalo_ref, got_ref, st_ref, dst_ref, msg_ref,
                 norm, norm_t, cf, dst, dacc, msg):
    t = pl.program_id(0)
    index = idx_ref[0]

    @pl.when(t == 0)
    def _():
        dacc[...] = jnp.zeros_like(dacc)
        run = jnp.zeros((2, 128), F32)
        nrun = jnp.zeros((1, 128), F32)
        for s in range(64):
            msg[s, 0:2, :] = run
            run = run + got_ref[s, 0:2, :]
            nrun = nrun + jnp.where(s < index, got_ref[s, 2:3, :], 0.0)
        norm[...] = jnp.broadcast_to(nrun, (128, 128)).T
        norm_t[...] = norm[...] - nhalo_ref[...]

    @pl.when(t > 0)
    def _():
        norm_t[...] = norm[...] + nloc_ref[0]

    feat = raw_ref[0, 0]
    decay = raw_ref[0, 2]
    rinv = 1.0 / (raw_ref[0, 3] + decay * per_head_sum(feat * norm_t[...]))
    coef = decay * rinv
    cf[...] = feat * coef
    for h in range(HEADS):
        dst[of(h), :] = folded(dot(stacked(cf[of(h), :]), ch_ref[h]))
    st_ref[0, 0] = coef
    st_ref[0, 1] = rinv
    st_ref[0, 2] = norm_t[...]
    dst_ref[0] = dst[...]
    dacc[...] += dst[...]

    @pl.when(t == 3)
    def _():
        for s in range(64):
            msg[s, 2:4, :] = dacc[2 * s : 2 * s + 2, :]
        msg_ref[...] = msg[...]


def state_kernel(raw_ref, st_ref, ch_ref, local_ref, halo_ref, got_ref, state_ref, pre_ref, dn_ref,
                 msg_ref, far, state, grad, drow, msg):
    t = pl.program_id(0)

    @pl.when(t == 0)
    def _():
        drow[...] = jnp.zeros_like(drow)
        run = jnp.zeros((2, 128), F32)
        for s in reversed(range(64)):
            far[2 * s : 2 * s + 2, :] = got_ref[s, 0:2, :]
            msg[s, 0:2, :] = run
            run = run + got_ref[s, 2:4, :]
        state[...] = far[...] - halo_ref[0]

    @pl.when(t > 0)
    def _():
        state[...] = far[...] + local_ref[0]

    for h in range(HEADS):
        grad[of(h), :] = folded(dot(stacked(state[of(h), :]), ch_ref[h], NT))
    state_ref[0] = state[...]
    coef = st_ref[0, 0]
    cf = raw_ref[0, 0] * coef
    along = raw_ref[0, 4] * st_ref[0, 1] + per_head_sum(cf * grad[...])
    pre_ref[0] = coef * (grad[...] - along * st_ref[0, 2]) * raw_ref[0, 1]
    dn = -(cf * along)
    dn_ref[0] = lane_sums(dn)
    drow[...] += row_sums(dn)

    @pl.when(t == 3)
    def _():
        for s in range(64):
            msg[s, 2:4, :] = drow[0:2, :]
        msg_ref[...] = msg[...]


def output_kernel(numer_ref, raw_ref, st_ref, state_ref, pre_ref, qh_ref, out_ref, gq_ref, cf,
                  rinv, state, pre, out, gq):
    t = pl.program_id(0)

    @pl.when(t == 0)
    def _():
        gq[...] = jnp.zeros_like(gq)

    cf[...] = raw_ref[0, 0] * st_ref[0, 0]
    rinv[...] = st_ref[0, 1]
    state[...] = state_ref[0]
    pre[...] = pre_ref[0]
    sub = lax.broadcasted_iota(jnp.int32, (RANK, TILE), 0)
    ones = jnp.ones((RANK, DH), F32)
    zeros = jnp.zeros((RANK, DH), F32)
    for h in range(HEADS):
        s = state[of(h), :]
        s_hi = s.astype(BF16).astype(F32)
        s_lo = s - s_hi
        c = cf[of(h), :]
        c_hi = c.astype(BF16).astype(F32)
        r = rinv[of(h), :]
        r_hi = r.astype(BF16).astype(F32)
        r_mid = (r - r_hi).astype(BF16).astype(F32)
        pieces = jnp.where(sub == 0, r_hi, jnp.where(sub == 1, r_mid, r - r_hi - r_mid))
        pieces = jnp.where(sub < 3, pieces, 0.0)
        lhs = jnp.concatenate([c_hi, c - c_hi, c_hi, pieces], 0).astype(BF16)
        left = jnp.concatenate([s_hi, s_hi, s_lo, zeros], 0)
        right = jnp.concatenate([zeros, zeros, zeros, ones], 0)
        both = dot(lhs, jnp.concatenate([left, right], 1).astype(BF16), TN)
        out[h] = (numer_ref[h] * both[:, DH:] + both[:, :DH]).astype(BF16)
        gq[of(h), :] += folded(dot(stacked(pre[of(h), :]), qh_ref[h]))
    out_ref[0] = jnp.swapaxes(out[...], 0, 1)

    @pl.when(t == 3)
    def _():
        gq_ref[...] = gq[...]


def key_grad_kernel(idx_ref, kh_ref, vh_ref, sig_ref, evict_ref, dst_ref, dn_ref, halo_in,
                    halo_ref, got_ref, gq_ref, out_ref, acc, nacc, grad, ev, near, gk):
    i = pl.program_id(0)
    n = 3 - i
    index = idx_ref[0]

    @pl.when(i == 0)
    def _():
        nrun = jnp.zeros((1, 128), F32)
        for s in range(64):
            acc[2 * s : 2 * s + 2, :] = got_ref[s, 0:2, :]
            nrun = nrun + jnp.where(s > index, got_ref[s, 2:3, :], 0.0)
        nacc[...] = jnp.broadcast_to(nrun, (128, 128)).T
        near[...] = dst_ref[0]
        for h in range(HEADS):
            grad[of(h), :] = folded(dot(stacked(near[of(h), :]), halo_in[1, h], NT))
        grad[...] = -(grad[...] + dn_ref[0]) * halo_ref[1]
        for h in range(HEADS):
            gk[of(h), :] = folded(dot(stacked(grad[of(h), :]), halo_in[0, h]))

    @pl.when(i >= 2)
    def _():
        acc[...] += dst_ref[jnp.minimum(n + 2, 3)]
        nacc[...] += dn_ref[jnp.minimum(n + 2, 3)]

    after = jnp.minimum(n + 1, 3)
    live = (n < 3).astype(F32)
    near[...] = dst_ref[after] * live
    for h in range(HEADS):
        res = dot(stacked(acc[of(h), :], near[of(h), :]), vh_ref[h], NT)
        grad[of(h), :] = folded(res)
        ev[of(h), :] = folded(res, 2 * RANK)
    grad[...] = (
        grad[...] + nacc[...] + evict_ref[0] * (ev[...] + dn_ref[after] * live)
    ) * sig_ref[0]
    for h in range(HEADS):
        gk[of(h), :] += folded(dot(stacked(grad[of(h), :]), kh_ref[h]))

    @pl.when(i == 3)
    def _():
        out_ref[:ROWS, :] = gq_ref[...]
        out_ref[ROWS:, :] = gk[...]


def spread_kernel(x_ref, o_ref):
    o_ref[...] = jnp.broadcast_to(jnp.sum(x_ref[...], 0, keepdims=True), o_ref.shape)


def sds(shape, dtype=F32):
    return jax.ShapeDtypeStruct(shape, dtype)


def whole(*shape):
    return pl.BlockSpec(shape, lambda *_: (0,) * len(shape))


def by_head(index):
    return pl.BlockSpec((HEADS, TILE, DH), lambda t: (0, index(t), 0))


def part(index, *lead):
    zeros = (0,) * (len(lead) + 2)
    return pl.BlockSpec((1, *lead, ROWS, TILE), lambda t: (index(t), *zeros))


def same(t):
    return t


def first(t):
    return 0


def prev(t):
    return jnp.maximum(t - 1, 0)


def back(t):
    return 3 - t


SMEM = pl.BlockSpec(memory_space=pltpu.SMEM)
ANY = pl.BlockSpec(memory_space=pl.ANY)
MAPS = whole(HEADS, RANK, DH)
MSG = whole(64, 4, 128)
MSG_T = sds((64, 4, 128))
MSG_S = pltpu.VMEM((64, 4, 128), F32)
NAT = pl.BlockSpec((1, TILE, HEADS, DH), lambda t: (0, t, 0, 0))
HALO = whole(2, HEADS, TILE, DH)
PAIR = whole(2, ROWS, TILE)
BIG = sds((HEADS, 4 * TILE, DH), BF16)
PARTS = sds((4, ROWS, TILE))
SQ = pltpu.VMEM((ROWS, TILE), F32)
HEAD_S = pltpu.VMEM((HEADS, TILE, DH), BF16)
ATTEND_S = [
    pltpu.VMEM((HEADS, 2 * TILE, TILE), F32),
    pltpu.VMEM((HEADS, 2 * TILE, TILE), BF16),
    pltpu.VMEM((HEADS, 2 * TILE, DH), BF16),
    SQ, SQ, SQ, SQ,
]


def exchanged(x, axes):
    return lax.all_to_all(x, axes, split_axis=0, concat_axis=0, tiled=True)


def call(kernel, name, grid, in_specs, out_specs, out_shape, scratch, us, aliases=None):
    return pl.pallas_call(
        kernel,
        grid=(grid,),
        in_specs=in_specs,
        out_specs=out_specs,
        out_shape=out_shape,
        scratch_shapes=scratch,
        name=name,
        input_output_aliases=aliases or {},
        cost_estimate=pl.CostEstimate(
            flops=int(us * 2e8), bytes_accessed=int(us * 1e6), transcendentals=0
        ),
        compiler_params=pltpu.CompilerParams(
            dimension_semantics=("arbitrary",), vmem_limit_bytes=VMEM
        ),
    )


def body(queries, keys, values, keep_count, query_map, key_map, cotangent):
    count = lax.axis_size(SEQ)
    steps = [(i, i + 1) for i in range(count - 1)]
    index = lax.axis_index(SEQ).astype(jnp.int32).reshape(1)
    counts = keep_count[0]
    qmap = query_map.transpose(0, 2, 1)
    kmap = key_map.transpose(0, 2, 1)

    kh, vh, edge, local, sig_k, evict, nloc, msg = call(
        keys_kernel, "keys", 4,
        [SMEM, SMEM, NAT, NAT, MAPS],
        [by_head(same), by_head(same), HALO, part(same), part(same), part(same), part(same), MSG],
        [BIG, BIG, sds((2, HEADS, TILE, DH), BF16), PARTS, PARTS, PARTS, PARTS, MSG_T],
        [SQ, SQ, SQ, SQ, SQ, SQ, pltpu.VMEM((2, ROWS, TILE), F32), MSG_S],
        4,
    )(index, counts, keys, values, kmap)

    halo_kv = lax.ppermute(edge, SEQ, steps)
    got = exchanged(msg, SEQ)

    qh, ch, numer, raw = call(
        near_kernel, "near", 4,
        [SMEM, SMEM, NAT, NAT, by_head(prev), by_head(same), by_head(prev), by_head(same), MAPS],
        [by_head(same), by_head(same), by_head(same), part(same, 5)],
        [BIG, BIG, sds((HEADS, 4 * TILE, DH)), sds((4, 5, ROWS, TILE))],
        [HEAD_S, HEAD_S, *ATTEND_S],
        8,
    )(index, counts, queries, cotangent, kh, kh, vh, vh, qmap)

    numer, raw, halo, nhalo = call(
        first_kernel, "first", 1,
        [SMEM, SMEM, by_head(first), by_head(first), HALO, by_head(first), by_head(first), MAPS,
         MAPS, ANY, ANY],
        [by_head(first), part(first, 5), PAIR, whole(ROWS, TILE)],
        [sds((HEADS, 4 * TILE, DH)), sds((4, 5, ROWS, TILE)), sds((2, ROWS, TILE)),
         sds((ROWS, TILE))],
        [HEAD_S, HEAD_S, SQ, SQ, *ATTEND_S],
        3,
        {9: 0, 10: 1},
    )(index, counts, qh, ch, halo_kv, kh, vh, qmap, kmap, numer, raw)

    st, dst, msg = call(
        total_kernel, "total", 4,
        [SMEM, part(same, 5), by_head(same), part(prev), whole(ROWS, TILE), MSG],
        [part(same, 3), part(same), MSG],
        [sds((4, 3, ROWS, TILE)), PARTS, MSG_T],
        [SQ, SQ, SQ, SQ, SQ, MSG_S],
        2,
    )(index, raw, ch, nloc, nhalo, got)

    got = exchanged(msg, SEQ)

    state, pre_q, dn, msg = call(
        state_kernel, "state", 4,
        [part(same, 5), part(same, 3), by_head(same), part(prev), PAIR, MSG],
        [part(same), part(same), part(same), MSG],
        [PARTS, PARTS, PARTS, MSG_T],
        [SQ, SQ, SQ, pltpu.VMEM((8, 128), F32), MSG_S],
        2,
    )(raw, st, ch, local, halo, got)

    got = exchanged(msg, SEQ)

    out, gq = call(
        output_kernel, "output", 4,
        [by_head(same), part(same, 5), part(same, 3), part(same), part(same), by_head(same)],
        [NAT, whole(ROWS, TILE)],
        [sds((1, 4 * TILE, HEADS, DH), BF16), sds((ROWS, TILE))],
        [SQ, SQ, SQ, SQ, HEAD_S, SQ],
        4,
    )(numer, raw, st, state, pre_q, qh)

    grads = call(
        key_grad_kernel, "key_grad", 4,
        [SMEM, by_head(back), by_head(back), part(back), part(back), whole(4, ROWS, TILE),
         whole(4, ROWS, TILE), HALO, PAIR, MSG, whole(ROWS, TILE)],
        whole(2 * ROWS, TILE),
        sds((2 * ROWS, TILE)),
        [SQ, SQ, SQ, SQ, SQ, SQ],
        3,
    )(index, kh, vh, sig_k, evict, dst, dn, halo_kv, halo, got, gq)

    spread = call(
        spread_kernel, "spread", 1, [whole(16, 16, 128)], whole(16, 16, 128), sds((16, 16, 128)),
        [], 1,
    )
    grads = exchanged(grads.reshape(16, 16, 128), ("z", "core"))
    grads = exchanged(spread(grads), ("y", "batch"))
    grads = exchanged(spread(grads), ("z", "core"))
    grad_q, grad_k = grads.reshape(2, HEADS, RANK, DH).transpose(0, 1, 3, 2)
    return out, grad_q, grad_k


def solution(mesh):
    torus = Mesh(mesh.devices.reshape(8, 4, 2, mesh.shape["batch"]), ALL)
    rows = P("batch", SEQ, None, None)
    in_specs = (rows, rows, rows, P("batch", None, None), P(), P(), rows)
    return jax.shard_map(
        body, mesh=torus, in_specs=in_specs, out_specs=(rows, P(), P()), check_vma=False
    )
```

```python
import math

import jax
import jax.numpy as jnp
from jax import lax
from jax.experimental import pallas as pl
from jax.experimental.pallas import tpu as pltpu
from jax.sharding import Mesh
from jax.sharding import PartitionSpec as P

TILE = 128
HEADS = 16
RANK = 8
DH = 128
ROWS = HEADS * RANK
SEQ = ("z", "y", "core")
ALL = ("z", "y", "core", "batch")
SHIFT = 1.5
SCALE = 1.0 / math.sqrt(DH)
SCALE_LOG2 = SCALE * math.log2(math.e)
NEG = -1e30
VMEM = 24 * 2**20
F32 = jnp.float32
BF16 = jnp.bfloat16
NN = (((1,), (0,)), ((), ()))
NT = (((1,), (1,)), ((), ()))
TN = (((0,), (0,)), ((), ()))


def dot(a, b, dims=NN):
    return lax.dot_general(a, b, dims, preferred_element_type=F32)


def halves(x):
    hi = x.astype(BF16)
    return hi, (x - hi.astype(F32)).astype(BF16)


def stacked(*parts):
    rows = []
    for x in parts:
        hi = x.astype(BF16).astype(F32)
        rows += [hi, x - hi]
    return jnp.concatenate(rows, 0).astype(BF16)


def folded(x, at=0):
    return x[at : at + RANK] + x[at + RANK : at + 2 * RANK]


def row_sums(x):
    ones = jnp.ones((8, 128), BF16)
    hi, lo = halves(x)
    return dot(ones, hi, NT) + dot(ones, lo, NT)


def softplus_sigmoid(pre):
    e = jnp.exp(-jnp.abs(pre))
    value = jnp.maximum(pre, 0.0) + jnp.log1p(e)
    inv = 1.0 / (1.0 + e)
    return value, jnp.where(pre >= 0, inv, e * inv)


def per_head_sum(x):
    x = x.reshape(HEADS, RANK, TILE)
    x = jnp.broadcast_to(jnp.sum(x, 1, keepdims=True), x.shape)
    return x.reshape(ROWS, TILE)


def of(h):
    return pl.ds(h * RANK, RANK)


def lane_sums(x):
    return jnp.broadcast_to(jnp.sum(x, 1, keepdims=True), (ROWS, TILE))


def keys_kernel(idx_ref, cnt_ref, k_ref, v_ref, kmap_ref, kh_ref, vh_ref, edge_ref, local_ref,
                sig_ref, evict_ref, nloc_ref, msg_ref, pre, evict, st_all, st_ev, all_acc, nacc,
                feats, msg, kbuf, vbuf, ksem, vsem):
    n = pl.program_id(0)

    def copies(m):
        rows = pl.ds(m * TILE, TILE)
        return (
            pltpu.make_async_copy(k_ref.at[0, rows], kbuf.at[m], ksem.at[m]),
            pltpu.make_async_copy(v_ref.at[0, rows], vbuf.at[m], vsem.at[m]),
        )

    @pl.when(n == 0)
    def _():
        for m in range(4):
            for copy in copies(m):
                copy.start()
        all_acc[...] = jnp.zeros_like(all_acc)
        nacc[...] = jnp.zeros_like(nacc)

    for copy in copies(n):
        copy.wait()
    kh_ref[...] = jnp.swapaxes(kbuf[n], 0, 1)
    vh_ref[...] = jnp.swapaxes(vbuf[n], 0, 1)
    lanes = lax.broadcasted_iota(jnp.int32, (RANK, TILE), 1)
    for h in range(HEADS):
        pre[of(h), :] = dot(kmap_ref[h], kh_ref[h], NT)
        count = cnt_ref[h, idx_ref[0] * 4 + n]
        evict[of(h), :] = (lanes >= count).astype(F32)
    feat, sig = softplus_sigmoid(pre[...] - SHIFT)
    ev = feat * evict[...]
    feats[0] = feat
    feats[1] = ev
    for h in range(HEADS):
        res = dot(stacked(feats[0, of(h), :], feats[1, of(h), :]), vh_ref[h])
        st_all[of(h), :] = folded(res)
        st_ev[of(h), :] = folded(res, 2 * RANK)
    evict_ref[0] = evict[...]
    sig_ref[0] = sig
    local_ref[0] = all_acc[...] + st_ev[...]
    all_acc[...] += st_all[...]
    nloc_ref[0] = lane_sums(ev) + nacc[...]
    nacc[...] += lane_sums(feat)

    @pl.when(n == 3)
    def _():
        edge_ref[0] = kh_ref[...]
        edge_ref[1] = vh_ref[...]
        row = row_sums(nacc[...] * (1.0 / 128.0))
        for s in range(64):
            msg[s, 0:2, :] = all_acc[2 * s : 2 * s + 2, :]
            msg[s, 2:4, :] = row[0:2]
        msg_ref[...] = msg[...]


def attention(kp_ref, ko_ref, vp_ref, vo_ref, qmap_ref, count_of, qs, cs, raw_ref, numer_ref,
              scores, weights, vv, pre, mx, den, cn):
    zeros = jnp.zeros((RANK, DH), F32)
    for h in range(HEADS):
        vv[h, 0:TILE, :] = vp_ref[h]
        vv[h, TILE:, :] = vo_ref[h]
        top = jnp.concatenate([qmap_ref[h].astype(F32), zeros], 0).astype(BF16)
        res = dot(jnp.concatenate([top, kp_ref[h], ko_ref[h]], 0), qs[h], NT)
        pre[of(h), :] = res[:RANK]
        scores[h] = res[2 * RANK :]
    rows = lax.broadcasted_iota(jnp.int32, (TILE, TILE), 0)
    cols = lax.broadcasted_iota(jnp.int32, (TILE, TILE), 1)
    causal = rows <= cols
    for h in range(HEADS):
        s_prev = jnp.where(rows < count_of(h), scores[h, 0:TILE, :], NEG)
        s_own = jnp.where(causal, scores[h, TILE:, :], NEG)
        top = jnp.max(jnp.maximum(s_prev, s_own), 0, keepdims=True)
        w_prev = jnp.exp2((s_prev - top) * SCALE_LOG2)
        w_own = jnp.exp2((s_own - top) * SCALE_LOG2)
        weights[h, 0:TILE, :] = w_prev.astype(BF16)
        weights[h, TILE:, :] = w_own.astype(BF16)
        sums = jnp.sum(w_prev + w_own, 0, keepdims=True)
        mx[of(h), :] = jnp.broadcast_to(top, (RANK, TILE))
        den[of(h), :] = jnp.broadcast_to(sums, (RANK, TILE))
    for h in range(HEADS):
        w = weights[h]
        against = w.astype(F32) * dot(vv[h], cs[h], NT)
        cn[of(h), :] = jnp.broadcast_to(jnp.sum(against, 0, keepdims=True), (RANK, TILE))
        numer_ref[h] = dot(w, vv[h], TN)
    feat, sig = softplus_sigmoid(pre[...] - SHIFT)
    raw_ref[0, 0] = feat
    raw_ref[0, 1] = sig
    raw_ref[0, 2] = jnp.exp(-(mx[...] * SCALE))
    raw_ref[0, 3] = den[...]
    raw_ref[0, 4] = cn[...]


def attend_kernel(idx_ref, cnt_ref, q_ref, c_ref, ko_ref, vo_ref, edge_ref, qmap_ref, kmap_ref,
                  nloc_ref, got_ref, qh_ref, ch_ref, numer_ref, raw_ref, st_ref, dst_ref,
                  halo_ref, msg_ref, qs, cs, kp, vp, kept, norm, norm_t, cf, dst, dacc, msg,
                  *scratch):
    t = pl.program_id(0)
    index = idx_ref[0]
    pre = scratch[3]
    before = index * 4 + t - 1
    counts = [
        jnp.where(before >= 0, cnt_ref[h, jnp.maximum(before, 0)], 0) for h in range(HEADS)
    ]

    @pl.when(t == 0)
    def _():
        dacc[...] = jnp.zeros_like(dacc)
        run = jnp.zeros((2, 128), F32)
        nrun = jnp.zeros((1, 128), F32)
        for s in range(64):
            msg[s, 0:2, :] = run
            run = run + got_ref[s, 0:2, :]
            nrun = nrun + jnp.where(s < index, got_ref[s, 2:3, :], 0.0)
        norm[...] = jnp.broadcast_to(nrun, (128, 128)).T
        kp[...] = edge_ref[0]
        vp[...] = edge_ref[1]
        lanes = lax.broadcasted_iota(jnp.int32, (RANK, TILE), 1)
        for h in range(HEADS):
            pre[of(h), :] = dot(kmap_ref[h], kp[h], NT)
            kept[of(h), :] = (lanes < counts[h]).astype(F32)
        feat, sig = softplus_sigmoid(pre[...] - SHIFT)
        feat = feat * kept[...]
        cf[...] = feat
        for h in range(HEADS):
            dst[of(h), :] = folded(dot(stacked(cf[of(h), :]), vp[h]))
        halo_ref[0] = dst[...]
        halo_ref[1] = kept[...] * sig
        norm_t[...] = norm[...] - lane_sums(feat)

    @pl.when(t > 0)
    def _():
        norm_t[...] = norm[...] + nloc_ref[0]

    qs[...] = jnp.swapaxes(q_ref[0], 0, 1)
    cs[...] = jnp.swapaxes(c_ref[0], 0, 1)
    attention(kp, ko_ref, vp, vo_ref, qmap_ref, lambda h: counts[h], qs, cs, raw_ref, numer_ref,
              *scratch)
    qh_ref[...] = qs[...]
    ch_ref[...] = cs[...]
    kp[...] = ko_ref[...]
    vp[...] = vo_ref[...]
    feat = raw_ref[0, 0]
    decay = raw_ref[0, 2]
    rinv = 1.0 / (raw_ref[0, 3] + decay * per_head_sum(feat * norm_t[...]))
    coef = decay * rinv
    cf[...] = feat * coef
    for h in range(HEADS):
        dst[of(h), :] = folded(dot(stacked(cf[of(h), :]), cs[h]))
    st_ref[0, 0] = coef
    st_ref[0, 1] = rinv
    st_ref[0, 2] = norm_t[...]
    dst_ref[0] = dst[...]
    dacc[...] += dst[...]

    @pl.when(t == 3)
    def _():
        for s in range(64):
            msg[s, 2:4, :] = dacc[2 * s : 2 * s + 2, :]
        msg_ref[...] = msg[...]


def output_kernel(numer_ref, raw_ref, st_ref, qh_ref, ch_ref, local_ref, halo_ref, got_ref,
                  out_ref, gq_ref, dn_ref, msg_ref, far, state, grad, drow, msg, cf, rinv, out,
                  gq):
    t = pl.program_id(0)

    @pl.when(t == 0)
    def _():
        drow[...] = jnp.zeros_like(drow)
        gq[...] = jnp.zeros_like(gq)
        run = jnp.zeros((2, 128), F32)
        for s in reversed(range(64)):
            far[2 * s : 2 * s + 2, :] = got_ref[s, 0:2, :]
            msg[s, 0:2, :] = run
            run = run + got_ref[s, 2:4, :]
        state[...] = far[...] - halo_ref[0]

    @pl.when(t > 0)
    def _():
        state[...] = far[...] + local_ref[0]

    coef = st_ref[0, 0]
    cf[...] = raw_ref[0, 0] * coef
    rinv[...] = st_ref[0, 1]
    sub = lax.broadcasted_iota(jnp.int32, (RANK, TILE), 0)
    ones = jnp.ones((RANK, DH), F32)
    zeros = jnp.zeros((RANK, DH), F32)
    for h in range(HEADS):
        s = state[of(h), :]
        s_hi = s.astype(BF16).astype(F32)
        s_lo = s - s_hi
        c = cf[of(h), :]
        c_hi = c.astype(BF16).astype(F32)
        r = rinv[of(h), :]
        r_hi = r.astype(BF16).astype(F32)
        r_mid = (r - r_hi).astype(BF16).astype(F32)
        pieces = jnp.where(sub == 0, r_hi, jnp.where(sub == 1, r_mid, r - r_hi - r_mid))
        pieces = jnp.where(sub < 3, pieces, 0.0)
        grad[of(h), :] = folded(dot(stacked(s), ch_ref[h], NT))
        lhs = jnp.concatenate([c_hi, c - c_hi, c_hi, pieces], 0).astype(BF16)
        left = jnp.concatenate([s_hi, s_hi, s_lo, zeros], 0)
        right = jnp.concatenate([zeros, zeros, zeros, ones], 0)
        both = dot(lhs, jnp.concatenate([left, right], 1).astype(BF16), TN)
        out[h] = (numer_ref[h] * both[:, DH:] + both[:, :DH]).astype(BF16)
    along = raw_ref[0, 4] * rinv[...] + per_head_sum(cf[...] * grad[...])
    dn = -(cf[...] * along)
    grad[...] = coef * (grad[...] - along * st_ref[0, 2]) * raw_ref[0, 1]
    for h in range(HEADS):
        gq[of(h), :] += folded(dot(stacked(grad[of(h), :]), qh_ref[h]))
    out_ref[0] = jnp.swapaxes(out[...], 0, 1)
    dn_ref[0] = lane_sums(dn)
    drow[...] += row_sums(dn)

    @pl.when(t == 3)
    def _():
        gq_ref[...] = gq[...]
        for s in range(64):
            msg[s, 2:4, :] = drow[0:2, :]
        msg_ref[...] = msg[...]


def key_grad_kernel(idx_ref, kh_ref, vh_ref, sig_ref, evict_ref, dst_ref, dn_ref, halo_in,
                    halo_ref, got_ref, gq_ref, out_ref, acc, nacc, grad, ev, near, gk):
    i = pl.program_id(0)
    n = 3 - i
    index = idx_ref[0]

    @pl.when(i == 0)
    def _():
        nrun = jnp.zeros((1, 128), F32)
        for s in range(64):
            acc[2 * s : 2 * s + 2, :] = got_ref[s, 0:2, :]
            nrun = nrun + jnp.where(s > index, got_ref[s, 2:3, :], 0.0)
        nacc[...] = jnp.broadcast_to(nrun, (128, 128)).T
        near[...] = dst_ref[0]
        for h in range(HEADS):
            grad[of(h), :] = folded(dot(stacked(near[of(h), :]), halo_in[1, h], NT))
        grad[...] = -(grad[...] + dn_ref[0]) * halo_ref[1]
        for h in range(HEADS):
            gk[of(h), :] = folded(dot(stacked(grad[of(h), :]), halo_in[0, h]))

    @pl.when(i >= 2)
    def _():
        acc[...] += dst_ref[jnp.minimum(n + 2, 3)]
        nacc[...] += dn_ref[jnp.minimum(n + 2, 3)]

    after = jnp.minimum(n + 1, 3)
    live = (n < 3).astype(F32)
    near[...] = dst_ref[after] * live
    for h in range(HEADS):
        res = dot(stacked(acc[of(h), :], near[of(h), :]), vh_ref[h], NT)
        grad[of(h), :] = folded(res)
        ev[of(h), :] = folded(res, 2 * RANK)
    grad[...] = (
        grad[...] + nacc[...] + evict_ref[0] * (ev[...] + dn_ref[after] * live)
    ) * sig_ref[0]
    for h in range(HEADS):
        gk[of(h), :] += folded(dot(stacked(grad[of(h), :]), kh_ref[h]))

    @pl.when(i == 3)
    def _():
        out_ref[:ROWS, :] = gq_ref[...]
        out_ref[ROWS:, :] = gk[...]


def spread_kernel(x_ref, o_ref):
    o_ref[...] = jnp.broadcast_to(jnp.sum(x_ref[...], 0, keepdims=True), o_ref.shape)


def sds(shape, dtype=F32):
    return jax.ShapeDtypeStruct(shape, dtype)


def whole(*shape):
    return pl.BlockSpec(shape, lambda *_: (0,) * len(shape))


def by_head(index):
    return pl.BlockSpec((HEADS, TILE, DH), lambda t: (0, index(t), 0))


def part(index, *lead):
    zeros = (0,) * (len(lead) + 2)
    return pl.BlockSpec((1, *lead, ROWS, TILE), lambda t: (index(t), *zeros))


def same(t):
    return t


def prev(t):
    return jnp.maximum(t - 1, 0)


def back(t):
    return 3 - t


SMEM = pl.BlockSpec(memory_space=pltpu.SMEM)
HBM = pl.BlockSpec(memory_space=pltpu.HBM)
TILES_S = pltpu.VMEM((4, TILE, HEADS, DH), BF16)
MAPS = whole(HEADS, RANK, DH)
MSG = whole(64, 4, 128)
MSG_T = sds((64, 4, 128))
MSG_S = pltpu.VMEM((64, 4, 128), F32)
NAT = pl.BlockSpec((1, TILE, HEADS, DH), lambda t: (0, t, 0, 0))
HALO = whole(2, HEADS, TILE, DH)
PAIR = whole(2, ROWS, TILE)
BIG = sds((HEADS, 4 * TILE, DH), BF16)
PARTS = sds((4, ROWS, TILE))
SQ = pltpu.VMEM((ROWS, TILE), F32)
HEAD_S = pltpu.VMEM((HEADS, TILE, DH), BF16)
ATTEND_S = [
    pltpu.VMEM((HEADS, 2 * TILE, TILE), F32),
    pltpu.VMEM((HEADS, 2 * TILE, TILE), BF16),
    pltpu.VMEM((HEADS, 2 * TILE, DH), BF16),
    SQ, SQ, SQ, SQ,
]


def exchanged(x, axes):
    return lax.all_to_all(x, axes, split_axis=0, concat_axis=0, tiled=True)


def call(kernel, name, grid, in_specs, out_specs, out_shape, scratch, us):
    return pl.pallas_call(
        kernel,
        grid=(grid,),
        in_specs=in_specs,
        out_specs=out_specs,
        out_shape=out_shape,
        scratch_shapes=scratch,
        name=name,
        cost_estimate=pl.CostEstimate(
            flops=int(us * 2e8), bytes_accessed=int(us * 1e6), transcendentals=0
        ),
        compiler_params=pltpu.CompilerParams(
            dimension_semantics=("arbitrary",), vmem_limit_bytes=VMEM
        ),
    )


def body(queries, keys, values, keep_count, query_map, key_map, cotangent):
    count = lax.axis_size(SEQ)
    steps = [(i, i + 1) for i in range(count - 1)]
    index = lax.axis_index(SEQ).astype(jnp.int32).reshape(1)
    counts = keep_count[0]
    qmap = query_map.transpose(0, 2, 1)
    kmap = key_map.transpose(0, 2, 1)

    kh, vh, edge, local, sig_k, evict, nloc, msg = call(
        keys_kernel, "keys", 4,
        [SMEM, SMEM, HBM, HBM, MAPS],
        [by_head(same), by_head(same), HALO, part(same), part(same), part(same), part(same), MSG],
        [BIG, BIG, sds((2, HEADS, TILE, DH), BF16), PARTS, PARTS, PARTS, PARTS, MSG_T],
        [SQ, SQ, SQ, SQ, SQ, SQ, pltpu.VMEM((2, ROWS, TILE), F32), MSG_S,
         TILES_S, TILES_S, pltpu.SemaphoreType.DMA((4,)), pltpu.SemaphoreType.DMA((4,))],
        4,
    )(index, counts, keys, values, kmap)

    edge = lax.ppermute(edge, SEQ, steps)
    got = exchanged(msg, SEQ)

    qh, ch, numer, raw, st, dst, halo, msg = call(
        attend_kernel, "attend", 4,
        [SMEM, SMEM, NAT, NAT, by_head(same), by_head(same), HALO, MAPS, MAPS,
         part(prev), MSG],
        [by_head(same), by_head(same), by_head(same), part(same, 5), part(same, 3), part(same),
         PAIR, MSG],
        [BIG, BIG, sds((HEADS, 4 * TILE, DH)), sds((4, 5, ROWS, TILE)), sds((4, 3, ROWS, TILE)),
         PARTS, sds((2, ROWS, TILE)), MSG_T],
        [HEAD_S, HEAD_S, HEAD_S, HEAD_S, SQ, SQ, SQ, SQ, SQ, SQ, MSG_S, *ATTEND_S],
        10,
    )(index, counts, queries, cotangent, kh, vh, edge, qmap, kmap, nloc, got)

    got = exchanged(msg, SEQ)

    out, gq, dn, msg = call(
        output_kernel, "output", 4,
        [by_head(same), part(same, 5), part(same, 3), by_head(same), by_head(same), part(prev),
         PAIR, MSG],
        [NAT, whole(ROWS, TILE), part(same), MSG],
        [sds((1, 4 * TILE, HEADS, DH), BF16), sds((ROWS, TILE)), PARTS, MSG_T],
        [SQ, SQ, SQ, pltpu.VMEM((8, 128), F32), MSG_S, SQ, SQ, HEAD_S, SQ],
        5,
    )(numer, raw, st, qh, ch, local, halo, got)

    got = exchanged(msg, SEQ)

    grads = call(
        key_grad_kernel, "key_grad", 4,
        [SMEM, by_head(back), by_head(back), part(back), part(back), whole(4, ROWS, TILE),
         whole(4, ROWS, TILE), HALO, PAIR, MSG, whole(ROWS, TILE)],
        whole(2 * ROWS, TILE),
        sds((2 * ROWS, TILE)),
        [SQ, SQ, SQ, SQ, SQ, SQ],
        3,
    )(index, kh, vh, sig_k, evict, dst, dn, edge, halo, got, gq)

    spread = call(
        spread_kernel, "spread", 1, [whole(16, 16, 128)], whole(16, 16, 128), sds((16, 16, 128)),
        [], 1,
    )
    grads = exchanged(grads.reshape(16, 16, 128), ("z", "core"))
    grads = exchanged(spread(grads), ("y", "batch"))
    grads = exchanged(spread(grads), ("z", "core"))
    grad_q, grad_k = grads.reshape(2, HEADS, RANK, DH).transpose(0, 1, 3, 2)
    return out, grad_q, grad_k


def solution(mesh):
    torus = Mesh(mesh.devices.reshape(8, 4, 2, mesh.shape["batch"]), ALL)
    rows = P("batch", SEQ, None, None)
    in_specs = (rows, rows, rows, P("batch", None, None), P(), P(), rows)
    return jax.shard_map(
        body, mesh=torus, in_specs=in_specs, out_specs=(rows, P(), P()), check_vma=False
    )
```

```python
import math

import jax
import jax.numpy as jnp
from jax import lax
from jax.experimental import pallas as pl
from jax.experimental.pallas import tpu as pltpu
from jax.sharding import Mesh
from jax.sharding import PartitionSpec as P

TILE = 128
HEADS = 16
RANK = 8
DH = 128
ROWS = HEADS * RANK
SEQ = ("z", "y", "core")
ALL = ("z", "y", "core", "batch")
SHIFT = 1.5
SCALE = 1.0 / math.sqrt(DH)
SCALE_LOG2 = SCALE * math.log2(math.e)
NEG = -1e30
VMEM = 24 * 2**20
F32 = jnp.float32
BF16 = jnp.bfloat16
NN = (((1,), (0,)), ((), ()))
NT = (((1,), (1,)), ((), ()))
TN = (((0,), (0,)), ((), ()))


def dot(a, b, dims=NN):
    return lax.dot_general(a, b, dims, preferred_element_type=F32)


def halves(x):
    hi = x.astype(BF16)
    return hi, (x - hi.astype(F32)).astype(BF16)


def stacked(*parts):
    rows = []
    for x in parts:
        hi = x.astype(BF16).astype(F32)
        rows += [hi, x - hi]
    return jnp.concatenate(rows, 0).astype(BF16)


def folded(x, at=0):
    return x[at : at + RANK] + x[at + RANK : at + 2 * RANK]


def row_sums(x):
    ones = jnp.ones((8, 128), BF16)
    hi, lo = halves(x)
    return dot(ones, hi, NT) + dot(ones, lo, NT)


def softplus_sigmoid(pre):
    e = jnp.exp(-jnp.abs(pre))
    value = jnp.maximum(pre, 0.0) + jnp.log1p(e)
    inv = 1.0 / (1.0 + e)
    return value, jnp.where(pre >= 0, inv, e * inv)


def per_head_sum(x):
    x = x.reshape(HEADS, RANK, TILE)
    x = jnp.broadcast_to(jnp.sum(x, 1, keepdims=True), x.shape)
    return x.reshape(ROWS, TILE)


def of(h):
    return pl.ds(h * RANK, RANK)


def lane_sums(x):
    return jnp.broadcast_to(jnp.sum(x, 1, keepdims=True), (ROWS, TILE))


def keys_kernel(idx_ref, cnt_ref, k_ref, v_ref, kmap_ref, kh_ref, vh_ref, edge_ref, local_ref,
                sig_ref, evict_ref, nloc_ref, msg_ref, pre, evict, st_all, st_ev, all_acc, nacc,
                tail, ntail, feats, msg):
    n = pl.program_id(0)
    tile = last_first(n)

    @pl.when(n == 0)
    def _():
        all_acc[...] = jnp.zeros_like(all_acc)
        nacc[...] = jnp.zeros_like(nacc)

    kh_ref[0] = jnp.swapaxes(k_ref[0], 0, 1)
    vh_ref[0] = jnp.swapaxes(v_ref[0], 0, 1)
    lanes = lax.broadcasted_iota(jnp.int32, (RANK, TILE), 1)
    for h in range(HEADS):
        pre[of(h), :] = dot(kmap_ref[h], kh_ref[0, h], NT)
        count = cnt_ref[h, idx_ref[0] * 4 + tile]
        evict[of(h), :] = (lanes >= count).astype(F32)
    feat, sig = softplus_sigmoid(pre[...] - SHIFT)
    ev = feat * evict[...]
    feats[0] = feat
    feats[1] = ev
    for h in range(HEADS):
        res = dot(stacked(feats[0, of(h), :], feats[1, of(h), :]), vh_ref[0, h])
        st_all[of(h), :] = folded(res)
        st_ev[of(h), :] = folded(res, 2 * RANK)
    evict_ref[0] = evict[...]
    sig_ref[0] = sig
    local_ref[0] = all_acc[...] + st_ev[...]
    nloc_ref[0] = lane_sums(ev) + nacc[...]

    @pl.when(n == 0)
    def _():
        edge_ref[0] = kh_ref[0]
        edge_ref[1] = vh_ref[0]
        tail[...] = st_all[...]
        ntail[...] = lane_sums(feat)

    @pl.when(n > 0)
    def _():
        all_acc[...] += st_all[...]
        nacc[...] += lane_sums(feat)

    @pl.when(n == 3)
    def _():
        all_acc[...] += tail[...]
        row = row_sums((nacc[...] + ntail[...]) * (1.0 / 128.0))
        for s in range(64):
            msg[s, 0:2, :] = all_acc[2 * s : 2 * s + 2, :]
            msg[s, 2:4, :] = row[0:2]
        msg_ref[...] = msg[...]


def attend_kernel(idx_ref, cnt_ref, q_ref, c_ref, ko_ref, vo_ref, edge_ref, qmap_ref, kmap_ref,
                  nloc_ref, got_ref, qh_ref, ch_ref, numer_ref, raw_ref, st_ref, dst_ref,
                  halo_ref, msg_ref, kp, vv, kept, norm, norm_t, cf, dst, dacc, msg, scores,
                  weights, pre, mx, den, cs):
    t = pl.program_id(0)
    index = idx_ref[0]
    before = index * 4 + t - 1
    counts = [
        jnp.where(before >= 0, cnt_ref[h, jnp.maximum(before, 0)], 0) for h in range(HEADS)
    ]
    own, other = t % 2, (t + 1) % 2

    @pl.when(t == 0)
    def _():
        dacc[...] = jnp.zeros_like(dacc)
        run = jnp.zeros((2, 128), F32)
        nrun = jnp.zeros((1, 128), F32)
        for s in range(64):
            msg[s, 0:2, :] = run
            run = run + got_ref[s, 0:2, :]
            nrun = nrun + jnp.where(s < index, got_ref[s, 2:3, :], 0.0)
        norm[...] = jnp.broadcast_to(nrun, (128, 128)).T
        kp[...] = edge_ref[0]
        vv[1] = edge_ref[1]
        lanes = lax.broadcasted_iota(jnp.int32, (RANK, TILE), 1)
        for h in range(HEADS):
            pre[of(h), :] = dot(kmap_ref[h], edge_ref[0, h], NT)
            kept[of(h), :] = (lanes < counts[h]).astype(F32)
        feat, sig = softplus_sigmoid(pre[...] - SHIFT)
        feat = feat * kept[...]
        cf[...] = feat
        for h in range(HEADS):
            dst[of(h), :] = folded(dot(stacked(cf[of(h), :]), edge_ref[1, h]))
        halo_ref[0] = dst[...]
        halo_ref[1] = kept[...] * sig
        norm_t[...] = norm[...] - lane_sums(feat)

    @pl.when(t > 0)
    def _():
        norm_t[...] = norm[...] + nloc_ref[0]

    qh_ref[0] = jnp.swapaxes(q_ref[0], 0, 1)
    cs[...] = jnp.swapaxes(c_ref[0], 0, 1)
    ch_ref[0] = cs[...]
    vv[own] = vo_ref[0]
    rows = lax.broadcasted_iota(jnp.int32, (TILE, TILE), 0)
    cols = lax.broadcasted_iota(jnp.int32, (TILE, TILE), 1)
    causal = rows <= cols
    zeros = jnp.zeros((RANK, DH), F32)
    for h in range(HEADS):
        top = jnp.concatenate([qmap_ref[h].astype(F32), zeros], 0).astype(BF16)
        res = dot(jnp.concatenate([top, kp[h], ko_ref[0, h]], 0), qh_ref[0, h], NT)
        pre[of(h), :] = res[:RANK]
        s_prev = jnp.where(rows < counts[h], res[2 * RANK : 2 * RANK + TILE], NEG)
        s_own = jnp.where(causal, res[2 * RANK + TILE :], NEG)
        scores[h, 0:TILE, :] = s_prev
        scores[h, TILE:, :] = s_own
        top = jnp.max(jnp.maximum(s_prev, s_own), 0, keepdims=True)
        mx[of(h), :] = jnp.broadcast_to(top, (RANK, TILE))
    kp[...] = ko_ref[0]
    for h in range(HEADS):
        s = scores[h].reshape(2 * TILE // RANK, RANK, TILE)
        w = jnp.exp2((s - mx[of(h), :][None]) * SCALE_LOG2)
        weights[h] = w.reshape(2 * TILE, TILE).astype(BF16)
        den[of(h), :] = jnp.sum(w, 0)
    along = jnp.zeros((TILE, ROWS), F32)
    for h in range(HEADS):
        v = jnp.concatenate([vv[other, h], vv[own, h]], 0)
        numer = dot(weights[h], v, TN)
        numer_ref[0, h] = numer
        sums = jnp.sum(numer * cs[h].astype(F32), 1, keepdims=True)
        along = jnp.where(cols == h * RANK, sums, along)
    cn = along.T
    feat, sig = softplus_sigmoid(pre[...] - SHIFT)
    decay = jnp.exp(-(mx[...] * SCALE))
    rinv = 1.0 / per_head_sum(den[...] + decay * feat * norm_t[...])
    coef = decay * rinv
    cf[...] = feat * coef
    for h in range(HEADS):
        dst[of(h), :] = folded(dot(stacked(cf[of(h), :]), cs[h]))
    st_ref[0, 0] = coef
    st_ref[0, 1] = rinv
    st_ref[0, 2] = norm_t[...]
    raw_ref[0, 0] = feat
    raw_ref[0, 1] = sig
    raw_ref[0, 2] = cn
    dst_ref[0] = dst[...]
    dacc[...] += dst[...]

    @pl.when(t == 3)
    def _():
        for s in range(64):
            msg[s, 2:4, :] = dacc[2 * s : 2 * s + 2, :]
        msg_ref[...] = msg[...]


def output_kernel(numer_ref, raw_ref, st_ref, qh_ref, ch_ref, local_ref, halo_ref, got_ref,
                  out_ref, gq_ref, dn_ref, msg_ref, far, state, grad, drow, msg, cf, rinv, out,
                  gq):
    t = pl.program_id(0)

    @pl.when(t == 0)
    def _():
        drow[...] = jnp.zeros_like(drow)
        gq[...] = jnp.zeros_like(gq)
        run = jnp.zeros((2, 128), F32)
        for s in reversed(range(64)):
            far[2 * s : 2 * s + 2, :] = got_ref[s, 0:2, :]
            msg[s, 0:2, :] = run
            run = run + got_ref[s, 2:4, :]
        state[...] = far[...] - halo_ref[0]

    @pl.when(t > 0)
    def _():
        state[...] = far[...] + local_ref[0]

    coef = st_ref[0, 0]
    cf[...] = raw_ref[0, 0] * coef
    rinv[...] = st_ref[0, 1]
    sub = lax.broadcasted_iota(jnp.int32, (RANK, TILE), 0)
    ones = jnp.ones((RANK, DH), F32)
    zeros = jnp.zeros((RANK, DH), F32)
    for h in range(HEADS):
        s = state[of(h), :]
        s_hi = s.astype(BF16).astype(F32)
        s_lo = s - s_hi
        c = cf[of(h), :]
        c_hi = c.astype(BF16).astype(F32)
        r = rinv[of(h), :]
        r_hi = r.astype(BF16).astype(F32)
        r_mid = (r - r_hi).astype(BF16).astype(F32)
        pieces = jnp.where(sub == 0, r_hi, jnp.where(sub == 1, r_mid, r - r_hi - r_mid))
        pieces = jnp.where(sub < 3, pieces, 0.0)
        grad[of(h), :] = folded(dot(stacked(s), ch_ref[0, h], NT))
        lhs = jnp.concatenate([c_hi, c - c_hi, c_hi, pieces], 0).astype(BF16)
        left = jnp.concatenate([s_hi, s_hi, s_lo, zeros], 0)
        right = jnp.concatenate([zeros, zeros, zeros, ones], 0)
        both = dot(lhs, jnp.concatenate([left, right], 1).astype(BF16), TN)
        out[h] = (numer_ref[0, h] * both[:, DH:] + both[:, :DH]).astype(BF16)
    along = per_head_sum(raw_ref[0, 2] * rinv[...] + cf[...] * grad[...])
    dn = -(cf[...] * along)
    grad[...] = coef * (grad[...] - along * st_ref[0, 2]) * raw_ref[0, 1]
    for h in range(HEADS):
        gq[of(h), :] += folded(dot(stacked(grad[of(h), :]), qh_ref[0, h]))
    out_ref[0] = jnp.swapaxes(out[...], 0, 1)
    dn_ref[0] = lane_sums(dn)
    drow[...] += row_sums(dn)

    @pl.when(t == 3)
    def _():
        gq_ref[...] = gq[...]
        for s in range(64):
            msg[s, 2:4, :] = drow[0:2, :]
        msg_ref[...] = msg[...]


def key_grad_kernel(idx_ref, kh_ref, vh_ref, sig_ref, evict_ref, dst_ref, dn_ref, halo_in,
                    halo_ref, got_ref, gq_ref, out_ref, acc, nacc, grad, ev, near, gk):
    i = pl.program_id(0)
    n = 3 - i
    index = idx_ref[0]

    @pl.when(i == 0)
    def _():
        nrun = jnp.zeros((1, 128), F32)
        for s in range(64):
            acc[2 * s : 2 * s + 2, :] = got_ref[s, 0:2, :]
            nrun = nrun + jnp.where(s > index, got_ref[s, 2:3, :], 0.0)
        nacc[...] = jnp.broadcast_to(nrun, (128, 128)).T
        near[...] = dst_ref[0]
        for h in range(HEADS):
            grad[of(h), :] = folded(dot(stacked(near[of(h), :]), halo_in[1, h], NT))
        grad[...] = -(grad[...] + dn_ref[0]) * halo_ref[1]
        for h in range(HEADS):
            gk[of(h), :] = folded(dot(stacked(grad[of(h), :]), halo_in[0, h]))

    @pl.when(i >= 2)
    def _():
        acc[...] += dst_ref[jnp.minimum(n + 2, 3)]
        nacc[...] += dn_ref[jnp.minimum(n + 2, 3)]

    after = jnp.minimum(n + 1, 3)
    live = (n < 3).astype(F32)
    near[...] = dst_ref[after] * live
    for h in range(HEADS):
        res = dot(stacked(acc[of(h), :], near[of(h), :]), vh_ref[0, h], NT)
        grad[of(h), :] = folded(res)
        ev[of(h), :] = folded(res, 2 * RANK)
    grad[...] = (
        grad[...] + nacc[...] + evict_ref[0] * (ev[...] + dn_ref[after] * live)
    ) * sig_ref[0]
    for h in range(HEADS):
        gk[of(h), :] += folded(dot(stacked(grad[of(h), :]), kh_ref[0, h]))

    @pl.when(i == 3)
    def _():
        out_ref[:ROWS, :] = gq_ref[...]
        out_ref[ROWS:, :] = gk[...]


def spread_kernel(x_ref, o_ref):
    o_ref[...] = jnp.broadcast_to(jnp.sum(x_ref[...], 0, keepdims=True), o_ref.shape)


def sds(shape, dtype=F32):
    return jax.ShapeDtypeStruct(shape, dtype)


def whole(*shape):
    return pl.BlockSpec(shape, lambda *_: (0,) * len(shape))


def by_head(index):
    return pl.BlockSpec((1, HEADS, TILE, DH), lambda t: (index(t), 0, 0, 0))


def part(index, *lead):
    zeros = (0,) * (len(lead) + 2)
    return pl.BlockSpec((1, *lead, ROWS, TILE), lambda t: (index(t), *zeros))


def natural(index):
    return pl.BlockSpec((1, TILE, HEADS, DH), lambda t: (0, index(t), 0, 0))


def last_first(t):
    return (t + 3) % 4


def same(t):
    return t


def prev(t):
    return jnp.maximum(t - 1, 0)


def back(t):
    return 3 - t


SMEM = pl.BlockSpec(memory_space=pltpu.SMEM)
MAPS = whole(HEADS, RANK, DH)
MSG = whole(64, 4, 128)
MSG_T = sds((64, 4, 128))
MSG_S = pltpu.VMEM((64, 4, 128), F32)
HALO = whole(2, HEADS, TILE, DH)
PAIR = whole(2, ROWS, TILE)
BIG = sds((4, HEADS, TILE, DH), BF16)
PARTS = sds((4, ROWS, TILE))
SQ = pltpu.VMEM((ROWS, TILE), F32)
HEAD_S = pltpu.VMEM((HEADS, TILE, DH), BF16)


def exchanged(x, axes):
    return lax.all_to_all(x, axes, split_axis=0, concat_axis=0, tiled=True)


def call(kernel, name, grid, in_specs, out_specs, out_shape, scratch, us, flags=None):
    return pl.pallas_call(
        kernel,
        grid=(grid,),
        in_specs=in_specs,
        out_specs=out_specs,
        out_shape=out_shape,
        scratch_shapes=scratch,
        name=name,
        cost_estimate=pl.CostEstimate(
            flops=int(us * 2e8), bytes_accessed=int(us * 1e6), transcendentals=0
        ),
        compiler_params=pltpu.CompilerParams(
            dimension_semantics=("arbitrary",), vmem_limit_bytes=VMEM, flags=flags
        ),
    )


def body(queries, keys, values, keep_count, query_map, key_map, cotangent):
    count = lax.axis_size(SEQ)
    steps = [(i, i + 1) for i in range(count - 1)]
    index = lax.axis_index(SEQ).astype(jnp.int32).reshape(1)
    counts = keep_count[0]
    qmap = query_map.transpose(0, 2, 1)
    kmap = key_map.transpose(0, 2, 1)

    kh, vh, edge, local, sig_k, evict, nloc, msg = call(
        keys_kernel, "keys", 4,
        [SMEM, SMEM, natural(last_first), natural(last_first), MAPS],
        [by_head(last_first), by_head(last_first), HALO, part(last_first), part(last_first),
         part(last_first), part(last_first), MSG],
        [BIG, BIG, sds((2, HEADS, TILE, DH), BF16), PARTS, PARTS, PARTS, PARTS, MSG_T],
        [SQ, SQ, SQ, SQ, SQ, SQ, SQ, SQ, pltpu.VMEM((2, ROWS, TILE), F32), MSG_S],
        4,
    )(index, counts, keys, values, kmap)

    edge = lax.ppermute(edge, SEQ, steps)
    got = exchanged(msg, SEQ)

    qh, ch, numer, raw, st, dst, halo, msg = call(
        attend_kernel, "attend", 4,
        [SMEM, SMEM, natural(same), natural(same), by_head(same), by_head(same), HALO, MAPS, MAPS,
         part(prev), MSG],
        [by_head(same), by_head(same), by_head(same), part(same, 3), part(same, 3), part(same),
         PAIR, MSG],
        [BIG, BIG, sds((4, HEADS, TILE, DH)), sds((4, 3, ROWS, TILE)), sds((4, 3, ROWS, TILE)),
         PARTS, sds((2, ROWS, TILE)), MSG_T],
        [HEAD_S, pltpu.VMEM((2, HEADS, TILE, DH), BF16), SQ, SQ, SQ, SQ, SQ, SQ, MSG_S,
         pltpu.VMEM((HEADS, 2 * TILE, TILE), F32), pltpu.VMEM((HEADS, 2 * TILE, TILE), BF16),
         SQ, SQ, SQ, HEAD_S],
        10,
    )(index, counts, queries, cotangent, kh, vh, edge, qmap, kmap, nloc, got)

    got = exchanged(msg, SEQ)

    out, gq, dn, msg = call(
        output_kernel, "output", 4,
        [by_head(same), part(same, 3), part(same, 3), by_head(same), by_head(same), part(prev),
         PAIR, MSG],
        [natural(same), whole(ROWS, TILE), part(same), MSG],
        [sds((1, 4 * TILE, HEADS, DH), BF16), sds((ROWS, TILE)), PARTS, MSG_T],
        [SQ, SQ, SQ, pltpu.VMEM((8, 128), F32), MSG_S, SQ, SQ, HEAD_S, SQ],
        5,
    )(numer, raw, st, qh, ch, local, halo, got)

    got = exchanged(msg, SEQ)

    grads = call(
        key_grad_kernel, "key_grad", 4,
        [SMEM, by_head(back), by_head(back), part(back), part(back), whole(4, ROWS, TILE),
         whole(4, ROWS, TILE), HALO, PAIR, MSG, whole(ROWS, TILE)],
        whole(2 * ROWS, TILE),
        sds((2 * ROWS, TILE)),
        [SQ, SQ, SQ, SQ, SQ, SQ],
        3,
    )(index, kh, vh, sig_k, evict, dst, dn, edge, halo, got, gq)

    spread = call(
        spread_kernel, "spread", 1, [whole(16, 16, 128)], whole(16, 16, 128), sds((16, 16, 128)),
        [], 1,
    )
    grads = exchanged(grads.reshape(16, 16, 128), ("z", "core"))
    grads = exchanged(spread(grads), ("y", "batch"))
    grads = exchanged(spread(grads), ("z", "core"))
    grad_q, grad_k = grads.reshape(2, HEADS, RANK, DH).transpose(0, 1, 3, 2)
    return out, grad_q, grad_k


def solution(mesh):
    torus = Mesh(mesh.devices.reshape(8, 4, 2, mesh.shape["batch"]), ALL)
    rows = P("batch", SEQ, None, None)
    in_specs = (rows, rows, rows, P("batch", None, None), P(), P(), rows)
    return jax.shard_map(
        body, mesh=torus, in_specs=in_specs, out_specs=(rows, P(), P()), check_vma=False
    )
```

```python
import math

import jax
import jax.numpy as jnp
from jax import lax
from jax.experimental import pallas as pl
from jax.experimental.pallas import tpu as pltpu
from jax.sharding import Mesh
from jax.sharding import PartitionSpec as P

TILE = 128
HEADS = 16
RANK = 8
DH = 128
ROWS = HEADS * RANK
SEQ = ("z", "y", "core")
ALL = ("z", "y", "core", "batch")
SHIFT = 1.5
SCALE = 1.0 / math.sqrt(DH)
SCALE_LOG2 = SCALE * math.log2(math.e)
NEG = -1e30
VMEM = 24 * 2**20
F32 = jnp.float32
BF16 = jnp.bfloat16
NN = (((1,), (0,)), ((), ()))
NT = (((1,), (1,)), ((), ()))
TN = (((0,), (0,)), ((), ()))


def dot(a, b, dims=NN):
    return lax.dot_general(a, b, dims, preferred_element_type=F32)


def halves(x):
    hi = x.astype(BF16)
    return hi, (x - hi.astype(F32)).astype(BF16)


def stacked(*parts):
    rows = []
    for x in parts:
        hi = x.astype(BF16).astype(F32)
        rows += [hi, x - hi]
    return jnp.concatenate(rows, 0).astype(BF16)


def folded(x, at=0):
    return x[at : at + RANK] + x[at + RANK : at + 2 * RANK]


def row_sums(x):
    ones = jnp.ones((8, 128), BF16)
    hi, lo = halves(x)
    return dot(ones, hi, NT) + dot(ones, lo, NT)


def softplus_sigmoid(pre):
    e = jnp.exp(-jnp.abs(pre))
    value = jnp.maximum(pre, 0.0) + jnp.log1p(e)
    inv = 1.0 / (1.0 + e)
    return value, jnp.where(pre >= 0, inv, e * inv)


def per_head_sum(x):
    x = x.reshape(HEADS, RANK, TILE)
    x = jnp.broadcast_to(jnp.sum(x, 1, keepdims=True), x.shape)
    return x.reshape(ROWS, TILE)


def of(h):
    return pl.ds(h * RANK, RANK)


def lane_sums(x):
    return jnp.broadcast_to(jnp.sum(x, 1, keepdims=True), (ROWS, TILE))


def keys_kernel(idx_ref, cnt_ref, k_ref, v_ref, kmap_ref, kh_ref, vh_ref, edge_ref, local_ref,
                sig_ref, evict_ref, nloc_ref, msg_ref, pre, evict, st_all, st_ev, all_acc, nacc,
                tail, ntail, feats, msg):
    n = pl.program_id(0)
    tile = last_first(n)

    @pl.when(n == 0)
    def _():
        all_acc[...] = jnp.zeros_like(all_acc)
        nacc[...] = jnp.zeros_like(nacc)

    kh_ref[0] = jnp.swapaxes(k_ref[0], 0, 1)
    vh_ref[0] = jnp.swapaxes(v_ref[0], 0, 1)
    lanes = lax.broadcasted_iota(jnp.int32, (RANK, TILE), 1)
    for h in range(HEADS):
        pre[of(h), :] = dot(kmap_ref[h], kh_ref[0, h], NT)
        count = cnt_ref[h, idx_ref[0] * 4 + tile]
        evict[of(h), :] = (lanes >= count).astype(F32)
    feat, sig = softplus_sigmoid(pre[...] - SHIFT)
    ev = feat * evict[...]
    feats[0] = feat
    feats[1] = ev
    for h in range(HEADS):
        res = dot(stacked(feats[0, of(h), :], feats[1, of(h), :]), vh_ref[0, h])
        st_all[of(h), :] = folded(res)
        st_ev[of(h), :] = folded(res, 2 * RANK)
    evict_ref[0] = evict[...]
    sig_ref[0] = sig
    local_ref[0] = all_acc[...] + st_ev[...]
    nloc_ref[0] = lane_sums(ev) + nacc[...]

    @pl.when(n == 0)
    def _():
        edge_ref[0] = kh_ref[0]
        edge_ref[1] = vh_ref[0]
        tail[...] = st_all[...]
        ntail[...] = lane_sums(feat)

    @pl.when(n > 0)
    def _():
        all_acc[...] += st_all[...]
        nacc[...] += lane_sums(feat)

    @pl.when(n == 3)
    def _():
        all_acc[...] += tail[...]
        row = row_sums((nacc[...] + ntail[...]) * (1.0 / 128.0))
        for s in range(64):
            msg[s, 0:2, :] = all_acc[2 * s : 2 * s + 2, :]
            msg[s, 2:4, :] = row[0:2]
        msg_ref[...] = msg[...]


def attend_kernel(idx_ref, cnt_ref, q_ref, c_ref, ko_ref, vo_ref, edge_ref, qmap_ref, kmap_ref,
                  nloc_ref, got_ref, qh_ref, ch_ref, numer_ref, raw_ref, st_ref, dst_ref,
                  halo_ref, msg_ref, kp, vv, kept, norm, norm_t, cf, dst, dacc, msg, scores,
                  weights, pre, mx, den, cs):
    t = pl.program_id(0)
    index = idx_ref[0]
    before = index * 4 + t - 1
    counts = [
        jnp.where(before >= 0, cnt_ref[h, jnp.maximum(before, 0)], 0) for h in range(HEADS)
    ]
    own, other = t % 2, (t + 1) % 2

    @pl.when(t == 0)
    def _():
        dacc[...] = jnp.zeros_like(dacc)
        run = jnp.zeros((2, 128), F32)
        nrun = jnp.zeros((1, 128), F32)
        for s in range(64):
            msg[s, 0:2, :] = run
            run = run + got_ref[s, 0:2, :]
            nrun = nrun + jnp.where(s < index, got_ref[s, 2:3, :], 0.0)
        norm[...] = jnp.broadcast_to(nrun, (128, 128)).T
        kp[...] = edge_ref[0]
        vv[1] = edge_ref[1]
        lanes = lax.broadcasted_iota(jnp.int32, (RANK, TILE), 1)
        for h in range(HEADS):
            pre[of(h), :] = dot(kmap_ref[h], edge_ref[0, h], NT)
            kept[of(h), :] = (lanes < counts[h]).astype(F32)
        feat, sig = softplus_sigmoid(pre[...] - SHIFT)
        feat = feat * kept[...]
        cf[...] = feat
        for h in range(HEADS):
            dst[of(h), :] = folded(dot(stacked(cf[of(h), :]), edge_ref[1, h]))
        halo_ref[0] = dst[...]
        halo_ref[1] = kept[...] * sig
        norm_t[...] = norm[...] - lane_sums(feat)

    @pl.when(t > 0)
    def _():
        norm_t[...] = norm[...] + nloc_ref[0]

    qh_ref[0] = jnp.swapaxes(q_ref[0], 0, 1)
    cs[...] = jnp.swapaxes(c_ref[0], 0, 1)
    ch_ref[0] = cs[...]
    vv[own] = vo_ref[0]
    rows = lax.broadcasted_iota(jnp.int32, (TILE, TILE), 0)
    cols = lax.broadcasted_iota(jnp.int32, (TILE, TILE), 1)
    causal = rows <= cols
    zeros = jnp.zeros((RANK, DH), F32)
    for h in range(HEADS):
        top = jnp.concatenate([qmap_ref[h].astype(F32), zeros], 0).astype(BF16)
        res = dot(jnp.concatenate([top, kp[h], ko_ref[0, h]], 0), qh_ref[0, h], NT)
        pre[of(h), :] = res[:RANK]
        s_prev = jnp.where(rows < counts[h], res[2 * RANK : 2 * RANK + TILE], NEG)
        s_own = jnp.where(causal, res[2 * RANK + TILE :], NEG)
        scores[h, 0:TILE, :] = s_prev
        scores[h, TILE:, :] = s_own
        top = jnp.max(jnp.maximum(s_prev, s_own), 0, keepdims=True)
        mx[of(h), :] = jnp.broadcast_to(top, (RANK, TILE))
    kp[...] = ko_ref[0]
    for h in range(HEADS):
        s = scores[h].reshape(2 * TILE // RANK, RANK, TILE)
        w = jnp.exp2((s - mx[of(h), :][None]) * SCALE_LOG2)
        weights[h] = w.reshape(2 * TILE, TILE).astype(BF16)
        den[of(h), :] = jnp.sum(w, 0)
    along = jnp.zeros((TILE, ROWS), F32)
    for h in range(HEADS):
        v = jnp.concatenate([vv[other, h], vv[own, h]], 0)
        numer = dot(weights[h], v, TN)
        numer_ref[0, h] = numer
        sums = jnp.sum(numer * cs[h].astype(F32), 1, keepdims=True)
        along = jnp.where(cols == h * RANK, sums, along)
    cn = along.T
    feat, sig = softplus_sigmoid(pre[...] - SHIFT)
    decay = jnp.exp(-(mx[...] * SCALE))
    rinv = 1.0 / per_head_sum(den[...] + decay * feat * norm_t[...])
    coef = decay * rinv
    cf[...] = feat * coef
    for h in range(HEADS):
        dst[of(h), :] = folded(dot(stacked(cf[of(h), :]), cs[h]))
    st_ref[0, 0] = coef
    st_ref[0, 1] = rinv
    st_ref[0, 2] = norm_t[...]
    raw_ref[0, 0] = feat
    raw_ref[0, 1] = sig
    raw_ref[0, 2] = cn
    dst_ref[0] = dst[...]
    dacc[...] += dst[...]

    @pl.when(t == 3)
    def _():
        for s in range(64):
            msg[s, 2:4, :] = dacc[2 * s : 2 * s + 2, :]
        msg_ref[...] = msg[...]


def output_kernel(numer_ref, raw_ref, st_ref, qh_ref, ch_ref, local_ref, halo_ref, got_ref,
                  out_ref, gq_ref, dn_ref, msg_ref, far, state, grad, drow, msg, cf, rinv, out,
                  gq):
    t = pl.program_id(0)

    @pl.when(t == 0)
    def _():
        drow[...] = jnp.zeros_like(drow)
        gq[...] = jnp.zeros_like(gq)
        run = jnp.zeros((2, 128), F32)
        for s in reversed(range(64)):
            far[2 * s : 2 * s + 2, :] = got_ref[s, 0:2, :]
            msg[s, 0:2, :] = run
            run = run + got_ref[s, 2:4, :]
        state[...] = far[...] - halo_ref[0]

    @pl.when(t > 0)
    def _():
        state[...] = far[...] + local_ref[0]

    coef = st_ref[0, 0]
    cf[...] = raw_ref[0, 0] * coef
    rinv[...] = st_ref[0, 1]
    sub = lax.broadcasted_iota(jnp.int32, (RANK, TILE), 0)
    ones = jnp.ones((RANK, DH), F32)
    zeros = jnp.zeros((RANK, DH), F32)
    for h in range(HEADS):
        s = state[of(h), :]
        s_hi = s.astype(BF16).astype(F32)
        s_lo = s - s_hi
        c = cf[of(h), :]
        c_hi = c.astype(BF16).astype(F32)
        r = rinv[of(h), :]
        r_hi = r.astype(BF16).astype(F32)
        r_mid = (r - r_hi).astype(BF16).astype(F32)
        pieces = jnp.where(sub == 0, r_hi, jnp.where(sub == 1, r_mid, r - r_hi - r_mid))
        pieces = jnp.where(sub < 3, pieces, 0.0)
        grad[of(h), :] = folded(dot(stacked(s), ch_ref[0, h], NT))
        lhs = jnp.concatenate([c_hi, c - c_hi, c_hi, pieces], 0).astype(BF16)
        left = jnp.concatenate([s_hi, s_hi, s_lo, zeros], 0)
        right = jnp.concatenate([zeros, zeros, zeros, ones], 0)
        both = dot(lhs, jnp.concatenate([left, right], 1).astype(BF16), TN)
        out[h] = (numer_ref[0, h] * both[:, DH:] + both[:, :DH]).astype(BF16)
    along = per_head_sum(raw_ref[0, 2] * rinv[...] + cf[...] * grad[...])
    dn = -(cf[...] * along)
    grad[...] = coef * (grad[...] - along * st_ref[0, 2]) * raw_ref[0, 1]
    for h in range(HEADS):
        gq[of(h), :] += folded(dot(stacked(grad[of(h), :]), qh_ref[0, h]))
    out_ref[0] = jnp.swapaxes(out[...], 0, 1)
    dn_ref[0] = lane_sums(dn)
    drow[...] += row_sums(dn)

    @pl.when(t == 3)
    def _():
        gq_ref[...] = gq[...]
        for s in range(64):
            msg[s, 2:4, :] = drow[0:2, :]
        msg_ref[...] = msg[...]


def key_grad_kernel(idx_ref, kh_ref, vh_ref, sig_ref, evict_ref, dst_ref, dn_ref, halo_in,
                    halo_ref, got_ref, gq_ref, out_ref, acc, nacc, grad, ev, near, gk):
    i = pl.program_id(0)
    n = 3 - i
    index = idx_ref[0]

    @pl.when(i == 0)
    def _():
        nrun = jnp.zeros((1, 128), F32)
        for s in range(64):
            acc[2 * s : 2 * s + 2, :] = got_ref[s, 0:2, :]
            nrun = nrun + jnp.where(s > index, got_ref[s, 2:3, :], 0.0)
        nacc[...] = jnp.broadcast_to(nrun, (128, 128)).T
        near[...] = dst_ref[0]
        for h in range(HEADS):
            grad[of(h), :] = folded(dot(stacked(near[of(h), :]), halo_in[1, h], NT))
        grad[...] = -(grad[...] + dn_ref[0]) * halo_ref[1]
        for h in range(HEADS):
            gk[of(h), :] = folded(dot(stacked(grad[of(h), :]), halo_in[0, h]))

    @pl.when(i >= 2)
    def _():
        acc[...] += dst_ref[jnp.minimum(n + 2, 3)]
        nacc[...] += dn_ref[jnp.minimum(n + 2, 3)]

    after = jnp.minimum(n + 1, 3)
    live = (n < 3).astype(F32)
    near[...] = dst_ref[after] * live
    for h in range(HEADS):
        res = dot(stacked(acc[of(h), :], near[of(h), :]), vh_ref[0, h], NT)
        grad[of(h), :] = folded(res)
        ev[of(h), :] = folded(res, 2 * RANK)
    grad[...] = (
        grad[...] + nacc[...] + evict_ref[0] * (ev[...] + dn_ref[after] * live)
    ) * sig_ref[0]
    for h in range(HEADS):
        gk[of(h), :] += folded(dot(stacked(grad[of(h), :]), kh_ref[0, h]))

    @pl.when(i == 3)
    def _():
        out_ref[:ROWS, :] = gq_ref[...]
        out_ref[ROWS:, :] = gk[...]


def spread_kernel(x_ref, o_ref):
    o_ref[...] = jnp.broadcast_to(jnp.sum(x_ref[...], 0, keepdims=True), o_ref.shape)


def sds(shape, dtype=F32):
    return jax.ShapeDtypeStruct(shape, dtype)


def whole(*shape):
    return pl.BlockSpec(shape, lambda *_: (0,) * len(shape))


def by_head(index):
    return pl.BlockSpec((1, HEADS, TILE, DH), lambda t: (index(t), 0, 0, 0))


def part(index, *lead):
    zeros = (0,) * (len(lead) + 2)
    return pl.BlockSpec((1, *lead, ROWS, TILE), lambda t: (index(t), *zeros))


def natural(index):
    return pl.BlockSpec((1, TILE, HEADS, DH), lambda t: (0, index(t), 0, 0))


def last_first(t):
    return (t + 3) % 4


def same(t):
    return t


def prev(t):
    return jnp.maximum(t - 1, 0)


def back(t):
    return 3 - t


SMEM = pl.BlockSpec(memory_space=pltpu.SMEM)
MAPS = whole(HEADS, RANK, DH)
MSG = whole(64, 4, 128)
MSG_T = sds((64, 4, 128))
MSG_S = pltpu.VMEM((64, 4, 128), F32)
HALO = whole(2, HEADS, TILE, DH)
PAIR = whole(2, ROWS, TILE)
BIG = sds((4, HEADS, TILE, DH), BF16)
PARTS = sds((4, ROWS, TILE))
SQ = pltpu.VMEM((ROWS, TILE), F32)
HEAD_S = pltpu.VMEM((HEADS, TILE, DH), BF16)


def exchanged(x, axes):
    return lax.all_to_all(x, axes, split_axis=0, concat_axis=0, tiled=True)


def call(kernel, name, grid, in_specs, out_specs, out_shape, scratch, us, flags=None):
    return pl.pallas_call(
        kernel,
        grid=(grid,),
        in_specs=in_specs,
        out_specs=out_specs,
        out_shape=out_shape,
        scratch_shapes=scratch,
        name=name,
        cost_estimate=pl.CostEstimate(
            flops=int(us * 2e8), bytes_accessed=int(us * 1e6), transcendentals=0
        ),
        compiler_params=pltpu.CompilerParams(
            dimension_semantics=("arbitrary",), vmem_limit_bytes=VMEM, flags=flags
        ),
    )


def body(queries, keys, values, keep_count, query_map, key_map, cotangent):
    count = lax.axis_size(SEQ)
    steps = [(i, i + 1) for i in range(count - 1)]
    index = lax.axis_index(SEQ).astype(jnp.int32).reshape(1)
    counts = keep_count[0]
    qmap = query_map.transpose(0, 2, 1)
    kmap = key_map.transpose(0, 2, 1)

    keys, values, kmap_now, counts_now = (
        pltpu.with_memory_space_constraint(x, pltpu.HBM) for x in (keys, values, kmap, counts)
    )
    kh, vh, edge, local, sig_k, evict, nloc, msg = call(
        keys_kernel, "keys", 4,
        [SMEM, SMEM, natural(last_first), natural(last_first), MAPS],
        [by_head(last_first), by_head(last_first), HALO, part(last_first), part(last_first),
         part(last_first), part(last_first), MSG],
        [BIG, BIG, sds((2, HEADS, TILE, DH), BF16), PARTS, PARTS, PARTS, PARTS, MSG_T],
        [SQ, SQ, SQ, SQ, SQ, SQ, SQ, SQ, pltpu.VMEM((2, ROWS, TILE), F32), MSG_S],
        4,
    )(index, counts_now, keys, values, kmap_now)

    edge = lax.ppermute(edge, SEQ, steps)
    got = exchanged(msg, SEQ)

    qh, ch, numer, raw, st, dst, halo, msg = call(
        attend_kernel, "attend", 4,
        [SMEM, SMEM, natural(same), natural(same), by_head(same), by_head(same), HALO, MAPS, MAPS,
         part(prev), MSG],
        [by_head(same), by_head(same), by_head(same), part(same, 3), part(same, 3), part(same),
         PAIR, MSG],
        [BIG, BIG, sds((4, HEADS, TILE, DH)), sds((4, 3, ROWS, TILE)), sds((4, 3, ROWS, TILE)),
         PARTS, sds((2, ROWS, TILE)), MSG_T],
        [HEAD_S, pltpu.VMEM((2, HEADS, TILE, DH), BF16), SQ, SQ, SQ, SQ, SQ, SQ, MSG_S,
         pltpu.VMEM((HEADS, 2 * TILE, TILE), F32), pltpu.VMEM((HEADS, 2 * TILE, TILE), BF16),
         SQ, SQ, SQ, HEAD_S],
        10,
    )(index, counts, queries, cotangent, kh, vh, edge, qmap, kmap, nloc, got)

    got = exchanged(msg, SEQ)

    out, gq, dn, msg = call(
        output_kernel, "output", 4,
        [by_head(same), part(same, 3), part(same, 3), by_head(same), by_head(same), part(prev),
         PAIR, MSG],
        [natural(same), whole(ROWS, TILE), part(same), MSG],
        [sds((1, 4 * TILE, HEADS, DH), BF16), sds((ROWS, TILE)), PARTS, MSG_T],
        [SQ, SQ, SQ, pltpu.VMEM((8, 128), F32), MSG_S, SQ, SQ, HEAD_S, SQ],
        5,
    )(numer, raw, st, qh, ch, local, halo, got)

    got = exchanged(msg, SEQ)

    grads = call(
        key_grad_kernel, "key_grad", 4,
        [SMEM, by_head(back), by_head(back), part(back), part(back), whole(4, ROWS, TILE),
         whole(4, ROWS, TILE), HALO, PAIR, MSG, whole(ROWS, TILE)],
        whole(2 * ROWS, TILE),
        sds((2 * ROWS, TILE)),
        [SQ, SQ, SQ, SQ, SQ, SQ],
        3,
    )(index, kh, vh, sig_k, evict, dst, dn, edge, halo, got, gq)

    spread = call(
        spread_kernel, "spread", 1, [whole(16, 16, 128)], whole(16, 16, 128), sds((16, 16, 128)),
        [], 1,
    )
    grads = exchanged(grads.reshape(16, 16, 128), ("z", "core"))
    grads = exchanged(spread(grads), ("y", "batch"))
    grads = exchanged(spread(grads), ("z", "core"))
    grad_q, grad_k = grads.reshape(2, HEADS, RANK, DH).transpose(0, 1, 3, 2)
    return out, grad_q, grad_k


def solution(mesh):
    torus = Mesh(mesh.devices.reshape(8, 4, 2, mesh.shape["batch"]), ALL)
    rows = P("batch", SEQ, None, None)
    in_specs = (rows, rows, rows, P("batch", None, None), P(), P(), rows)
    return jax.shard_map(
        body, mesh=torus, in_specs=in_specs, out_specs=(rows, P(), P()), check_vma=False
    )
```

```python
import math

import jax
import jax.numpy as jnp
from jax import lax
from jax.experimental import pallas as pl
from jax.experimental.pallas import tpu as pltpu
from jax.sharding import Mesh
from jax.sharding import PartitionSpec as P

TILE = 128
HEADS = 16
RANK = 8
DH = 128
ROWS = HEADS * RANK
SEQ = ("z", "y", "core")
ALL = ("z", "y", "core", "batch")
SHIFT = 1.5
SCALE = 1.0 / math.sqrt(DH)
SCALE_LOG2 = SCALE * math.log2(math.e)
NEG = -1e30
VMEM = 24 * 2**20
FULL = 67_043_328
F32 = jnp.float32
BF16 = jnp.bfloat16
NN = (((1,), (0,)), ((), ()))
NT = (((1,), (1,)), ((), ()))
TN = (((0,), (0,)), ((), ()))


def dot(a, b, dims=NN):
    return lax.dot_general(a, b, dims, preferred_element_type=F32)


def halves(x):
    hi = x.astype(BF16)
    return hi, (x - hi.astype(F32)).astype(BF16)


def stacked(*parts):
    rows = []
    for x in parts:
        hi = x.astype(BF16).astype(F32)
        rows += [hi, x - hi]
    return jnp.concatenate(rows, 0).astype(BF16)


def folded(x, at=0):
    return x[at : at + RANK] + x[at + RANK : at + 2 * RANK]


def row_sums(x):
    ones = jnp.ones((8, 128), BF16)
    hi, lo = halves(x)
    return dot(ones, hi, NT) + dot(ones, lo, NT)


def softplus_sigmoid(pre):
    e = jnp.exp(-jnp.abs(pre))
    value = jnp.maximum(pre, 0.0) + jnp.log1p(e)
    inv = 1.0 / (1.0 + e)
    return value, jnp.where(pre >= 0, inv, e * inv)


def per_head_sum(x):
    x = x.reshape(HEADS, RANK, TILE)
    x = jnp.broadcast_to(jnp.sum(x, 1, keepdims=True), x.shape)
    return x.reshape(ROWS, TILE)


def of(h):
    return pl.ds(h * RANK, RANK)


def lane_sums(x):
    return jnp.broadcast_to(jnp.sum(x, 1, keepdims=True), (ROWS, TILE))


def keys_kernel(idx_ref, cnt_ref, k_ref, v_ref, kmap_ref, kh_ref, vh_ref, edge_ref, local_ref,
                sig_ref, evict_ref, nloc_ref, msg_ref, pre, evict, st_all, st_ev, all_acc, nacc,
                tail, ntail, feats, msg):
    n = pl.program_id(0)
    tile = last_first(n)

    @pl.when(n == 0)
    def _():
        all_acc[...] = jnp.zeros_like(all_acc)
        nacc[...] = jnp.zeros_like(nacc)

    kh_ref[0] = jnp.swapaxes(k_ref[0], 0, 1)
    vh_ref[0] = jnp.swapaxes(v_ref[0], 0, 1)
    lanes = lax.broadcasted_iota(jnp.int32, (RANK, TILE), 1)
    for h in range(HEADS):
        pre[of(h), :] = dot(kmap_ref[h], kh_ref[0, h], NT)
        count = cnt_ref[h, idx_ref[0] * 4 + tile]
        evict[of(h), :] = (lanes >= count).astype(F32)
    feat, sig = softplus_sigmoid(pre[...] - SHIFT)
    ev = feat * evict[...]
    feats[0] = feat
    feats[1] = ev
    for h in range(HEADS):
        res = dot(stacked(feats[0, of(h), :], feats[1, of(h), :]), vh_ref[0, h])
        st_all[of(h), :] = folded(res)
        st_ev[of(h), :] = folded(res, 2 * RANK)
    evict_ref[0] = evict[...]
    sig_ref[0] = sig
    local_ref[0] = all_acc[...] + st_ev[...]
    nloc_ref[0] = lane_sums(ev) + nacc[...]

    @pl.when(n == 0)
    def _():
        edge_ref[0] = kh_ref[0]
        edge_ref[1] = vh_ref[0]
        tail[...] = st_all[...]
        ntail[...] = lane_sums(feat)

    @pl.when(n > 0)
    def _():
        all_acc[...] += st_all[...]
        nacc[...] += lane_sums(feat)

    @pl.when(n == 3)
    def _():
        all_acc[...] += tail[...]
        row = row_sums((nacc[...] + ntail[...]) * (1.0 / 128.0))
        for s in range(64):
            msg[s, 0:2, :] = all_acc[2 * s : 2 * s + 2, :]
            msg[s, 2:4, :] = row[0:2]
        msg_ref[...] = msg[...]


def attention(kp_ref, ko_ref, vp_ref, vo_ref, q_ref, c_ref, qmap_ref, count_of, numer_ref, raw,
              scores, weights, pre, mx, den, numer):
    rows = lax.broadcasted_iota(jnp.int32, (TILE, TILE), 0)
    cols = lax.broadcasted_iota(jnp.int32, (TILE, TILE), 1)
    causal = rows <= cols
    zeros = jnp.zeros((RANK, DH), F32)
    for h in range(HEADS):
        top = jnp.concatenate([qmap_ref[h].astype(F32), zeros], 0).astype(BF16)
        res = dot(jnp.concatenate([top, kp_ref[0, h], ko_ref[0, h]], 0), q_ref[0, h], NT)
        pre[of(h), :] = res[:RANK]
        s_prev = jnp.where(rows < count_of(h), res[2 * RANK : 2 * RANK + TILE], NEG)
        s_own = jnp.where(causal, res[2 * RANK + TILE :], NEG)
        scores[h, 0:TILE, :] = s_prev
        scores[h, TILE:, :] = s_own
        top = jnp.max(jnp.maximum(s_prev, s_own), 0, keepdims=True)
        mx[of(h), :] = jnp.broadcast_to(top, (RANK, TILE))
    for h in range(HEADS):
        s = scores[h].reshape(2 * TILE // RANK, RANK, TILE)
        w = jnp.exp2((s - mx[of(h), :][None]) * SCALE_LOG2)
        weights[h] = w.reshape(2 * TILE, TILE).astype(BF16)
        den[of(h), :] = jnp.sum(w, 0)
    along = jnp.zeros((TILE, ROWS), F32)
    for h in range(HEADS):
        v = jnp.concatenate([vp_ref[0, h], vo_ref[0, h]], 0)
        part = dot(weights[h], v, TN)
        numer[h] = part
        sums = jnp.sum(part * c_ref[0, h].astype(F32), 1, keepdims=True)
        along = jnp.where(cols == h * RANK, sums, along)
    numer_ref[0] = numer[...]
    feat, sig = softplus_sigmoid(pre[...] - SHIFT)
    raw[0, 0] = feat
    raw[0, 1] = sig
    raw[0, 2] = along.T
    raw[0, 3] = den[...]
    raw[0, 4] = jnp.exp(-(mx[...] * SCALE))


def near_kernel(idx_ref, cnt_ref, q_ref, c_ref, kp_ref, ko_ref, vp_ref, vo_ref, qmap_ref, qh_ref,
                ch_ref, numer_ref, raw_ref, *scratch):
    t = pl.program_id(0)
    qh_ref[0] = jnp.swapaxes(q_ref[0], 0, 1)
    ch_ref[0] = jnp.swapaxes(c_ref[0], 0, 1)

    @pl.when(t > 0)
    def _():
        before = idx_ref[0] * 4 + jnp.maximum(t - 1, 0)
        attention(kp_ref, ko_ref, vp_ref, vo_ref, qh_ref, ch_ref, qmap_ref,
                  lambda h: cnt_ref[h, before], numer_ref, raw_ref, *scratch)


def rest_kernel(idx_ref, cnt_ref, q0_ref, ch_ref, edge_ref, ko_ref, vo_ref, qmap_ref, kmap_ref,
                raw_ref, nloc_ref, got_ref, numer_any, numer_ref, st_ref, dst_ref, halo_ref,
                msg_ref, kept, norm, norm_t, cf, dst, dacc, msg, raw, *scratch):
    del numer_any
    t = pl.program_id(0)
    index = idx_ref[0]
    pre = scratch[2]

    @pl.when(t == 0)
    def _():
        dacc[...] = jnp.zeros_like(dacc)
        run = jnp.zeros((2, 128), F32)
        nrun = jnp.zeros((1, 128), F32)
        for s in range(64):
            msg[s, 0:2, :] = run
            run = run + got_ref[s, 0:2, :]
            nrun = nrun + jnp.where(s < index, got_ref[s, 2:3, :], 0.0)
        norm[...] = jnp.broadcast_to(nrun, (128, 128)).T
        before = jnp.maximum(index * 4 - 1, 0)
        counts = [jnp.where(index > 0, cnt_ref[h, before], 0) for h in range(HEADS)]
        lanes = lax.broadcasted_iota(jnp.int32, (RANK, TILE), 1)
        for h in range(HEADS):
            pre[of(h), :] = dot(kmap_ref[h], edge_ref[0, h], NT)
            kept[of(h), :] = (lanes < counts[h]).astype(F32)
        feat, sig = softplus_sigmoid(pre[...] - SHIFT)
        feat = feat * kept[...]
        cf[...] = feat
        for h in range(HEADS):
            dst[of(h), :] = folded(dot(stacked(cf[of(h), :]), edge_ref[1, h]))
        halo_ref[0] = dst[...]
        halo_ref[1] = kept[...] * sig
        norm_t[...] = norm[...] - lane_sums(feat)
        attention(edge_ref.at[0:1], ko_ref, edge_ref.at[1:2], vo_ref, q0_ref, ch_ref, qmap_ref,
                  lambda h: counts[h], numer_ref, raw, *scratch)

    @pl.when(t > 0)
    def _():
        norm_t[...] = norm[...] + nloc_ref[0]
        raw[...] = raw_ref[...]

    feat = raw[0, 0]
    decay = raw[0, 4]
    rinv = 1.0 / per_head_sum(raw[0, 3] + decay * feat * norm_t[...])
    coef = decay * rinv
    cf[...] = feat * coef
    for h in range(HEADS):
        dst[of(h), :] = folded(dot(stacked(cf[of(h), :]), ch_ref[0, h]))
    st_ref[0, 0] = coef
    st_ref[0, 1] = rinv
    st_ref[0, 2] = norm_t[...]
    st_ref[0, 3] = feat
    st_ref[0, 4] = raw[0, 1]
    st_ref[0, 5] = raw[0, 2]
    dst_ref[0] = dst[...]
    dacc[...] += dst[...]

    @pl.when(t == 3)
    def _():
        for s in range(64):
            msg[s, 2:4, :] = dacc[2 * s : 2 * s + 2, :]
        msg_ref[...] = msg[...]


def output_kernel(numer_ref, st_ref, qh_ref, ch_ref, local_ref, halo_ref, got_ref,
                  out_ref, gq_ref, dn_ref, msg_ref, far, state, grad, drow, msg, cf, rinv, out,
                  gq):
    t = pl.program_id(0)

    @pl.when(t == 0)
    def _():
        drow[...] = jnp.zeros_like(drow)
        gq[...] = jnp.zeros_like(gq)
        run = jnp.zeros((2, 128), F32)
        for s in reversed(range(64)):
            far[2 * s : 2 * s + 2, :] = got_ref[s, 0:2, :]
            msg[s, 0:2, :] = run
            run = run + got_ref[s, 2:4, :]
        state[...] = far[...] - halo_ref[0]

    @pl.when(t > 0)
    def _():
        state[...] = far[...] + local_ref[0]

    coef = st_ref[0, 0]
    cf[...] = st_ref[0, 3] * coef
    rinv[...] = st_ref[0, 1]
    sub = lax.broadcasted_iota(jnp.int32, (RANK, TILE), 0)
    ones = jnp.ones((RANK, DH), F32)
    zeros = jnp.zeros((RANK, DH), F32)
    for h in range(HEADS):
        s = state[of(h), :]
        s_hi = s.astype(BF16).astype(F32)
        s_lo = s - s_hi
        c = cf[of(h), :]
        c_hi = c.astype(BF16).astype(F32)
        r = rinv[of(h), :]
        r_hi = r.astype(BF16).astype(F32)
        r_mid = (r - r_hi).astype(BF16).astype(F32)
        pieces = jnp.where(sub == 0, r_hi, jnp.where(sub == 1, r_mid, r - r_hi - r_mid))
        pieces = jnp.where(sub < 3, pieces, 0.0)
        grad[of(h), :] = folded(dot(stacked(s), ch_ref[0, h], NT))
        lhs = jnp.concatenate([c_hi, c - c_hi, c_hi, pieces], 0).astype(BF16)
        left = jnp.concatenate([s_hi, s_hi, s_lo, zeros], 0)
        right = jnp.concatenate([zeros, zeros, zeros, ones], 0)
        both = dot(lhs, jnp.concatenate([left, right], 1).astype(BF16), TN)
        out[h] = (numer_ref[0, h] * both[:, DH:] + both[:, :DH]).astype(BF16)
    along = per_head_sum(st_ref[0, 5] * rinv[...] + cf[...] * grad[...])
    dn = -(cf[...] * along)
    grad[...] = coef * (grad[...] - along * st_ref[0, 2]) * st_ref[0, 4]
    for h in range(HEADS):
        gq[of(h), :] += folded(dot(stacked(grad[of(h), :]), qh_ref[0, h]))
    out_ref[0] = jnp.swapaxes(out[...], 0, 1)
    dn_ref[0] = lane_sums(dn)
    drow[...] += row_sums(dn)

    @pl.when(t == 3)
    def _():
        gq_ref[...] = gq[...]
        for s in range(64):
            msg[s, 2:4, :] = drow[0:2, :]
        msg_ref[...] = msg[...]


def key_grad_kernel(idx_ref, kh_ref, vh_ref, sig_ref, evict_ref, dst_ref, dn_ref, halo_in,
                    halo_ref, got_ref, gq_ref, out_ref, acc, nacc, grad, ev, near, gk):
    i = pl.program_id(0)
    n = 3 - i
    index = idx_ref[0]

    @pl.when(i == 0)
    def _():
        nrun = jnp.zeros((1, 128), F32)
        for s in range(64):
            acc[2 * s : 2 * s + 2, :] = got_ref[s, 0:2, :]
            nrun = nrun + jnp.where(s > index, got_ref[s, 2:3, :], 0.0)
        nacc[...] = jnp.broadcast_to(nrun, (128, 128)).T
        near[...] = dst_ref[0]
        for h in range(HEADS):
            grad[of(h), :] = folded(dot(stacked(near[of(h), :]), halo_in[1, h], NT))
        grad[...] = -(grad[...] + dn_ref[0]) * halo_ref[1]
        for h in range(HEADS):
            gk[of(h), :] = folded(dot(stacked(grad[of(h), :]), halo_in[0, h]))

    @pl.when(i >= 2)
    def _():
        acc[...] += dst_ref[jnp.minimum(n + 2, 3)]
        nacc[...] += dn_ref[jnp.minimum(n + 2, 3)]

    after = jnp.minimum(n + 1, 3)
    live = (n < 3).astype(F32)
    near[...] = dst_ref[after] * live
    for h in range(HEADS):
        res = dot(stacked(acc[of(h), :], near[of(h), :]), vh_ref[0, h], NT)
        grad[of(h), :] = folded(res)
        ev[of(h), :] = folded(res, 2 * RANK)
    grad[...] = (
        grad[...] + nacc[...] + evict_ref[0] * (ev[...] + dn_ref[after] * live)
    ) * sig_ref[0]
    for h in range(HEADS):
        gk[of(h), :] += folded(dot(stacked(grad[of(h), :]), kh_ref[0, h]))

    @pl.when(i == 3)
    def _():
        out_ref[:ROWS, :] = gq_ref[...]
        out_ref[ROWS:, :] = gk[...]


def spread_kernel(x_ref, o_ref):
    o_ref[...] = jnp.broadcast_to(jnp.sum(x_ref[...], 0, keepdims=True), o_ref.shape)


def sds(shape, dtype=F32):
    return jax.ShapeDtypeStruct(shape, dtype)


def whole(*shape):
    return pl.BlockSpec(shape, lambda *_: (0,) * len(shape))


def by_head(index):
    return pl.BlockSpec((1, HEADS, TILE, DH), lambda t: (index(t), 0, 0, 0))


def part(index, *lead):
    zeros = (0,) * (len(lead) + 2)
    return pl.BlockSpec((1, *lead, ROWS, TILE), lambda t: (index(t), *zeros))


def natural(index):
    return pl.BlockSpec((1, TILE, HEADS, DH), lambda t: (0, index(t), 0, 0))


def last_first(t):
    return (t + 3) % 4


def first(t):
    return 0


def same(t):
    return t


def prev(t):
    return jnp.maximum(t - 1, 0)


def back(t):
    return 3 - t


SMEM = pl.BlockSpec(memory_space=pltpu.SMEM)
ANY = pl.BlockSpec(memory_space=pl.ANY)
MAPS = whole(HEADS, RANK, DH)
MSG = whole(64, 4, 128)
MSG_T = sds((64, 4, 128))
MSG_S = pltpu.VMEM((64, 4, 128), F32)
HALO = whole(2, HEADS, TILE, DH)
PAIR = whole(2, ROWS, TILE)
BIG = sds((4, HEADS, TILE, DH), BF16)
PARTS = sds((4, ROWS, TILE))
SQ = pltpu.VMEM((ROWS, TILE), F32)
HEAD_S = pltpu.VMEM((HEADS, TILE, DH), BF16)


def hbm(*arrays):
    return jax.tree.map(lambda x: pltpu.with_memory_space_constraint(x, pltpu.HBM), arrays)


def exchanged(x, axes):
    return lax.all_to_all(x, axes, split_axis=0, concat_axis=0, tiled=True)


def call(kernel, name, grid, in_specs, out_specs, out_shape, scratch, us, vmem=VMEM, aliases=None):
    return pl.pallas_call(
        kernel,
        grid=(grid,),
        in_specs=in_specs,
        out_specs=out_specs,
        out_shape=out_shape,
        scratch_shapes=scratch,
        name=name,
        input_output_aliases=aliases or {},
        cost_estimate=pl.CostEstimate(
            flops=int(us * 2e8), bytes_accessed=int(us * 1e6), transcendentals=0
        ),
        compiler_params=pltpu.CompilerParams(
            dimension_semantics=("arbitrary",), vmem_limit_bytes=vmem
        ),
    )


def body(queries, keys, values, keep_count, query_map, key_map, cotangent):
    count = lax.axis_size(SEQ)
    steps = [(i, i + 1) for i in range(count - 1)]
    index = lax.axis_index(SEQ).astype(jnp.int32).reshape(1)
    counts = keep_count[0]
    qmap = query_map.transpose(0, 2, 1)
    kmap = key_map.transpose(0, 2, 1)

    kh, vh, edge, local, sig_k, evict, nloc, msg = call(
        keys_kernel, "keys", 4,
        [SMEM, SMEM, natural(last_first), natural(last_first), MAPS],
        [by_head(last_first), by_head(last_first), HALO, part(last_first), part(last_first),
         part(last_first), part(last_first), MSG],
        [BIG, BIG, sds((2, HEADS, TILE, DH), BF16), PARTS, PARTS, PARTS, PARTS, MSG_T],
        [SQ, SQ, SQ, SQ, SQ, SQ, SQ, SQ, pltpu.VMEM((2, ROWS, TILE), F32), MSG_S],
        4, FULL,
    )(index, counts, keys, values, kmap)

    edge = lax.ppermute(edge, SEQ, steps)
    got = exchanged(msg, SEQ)

    attend_scratch = [
        pltpu.VMEM((HEADS, 2 * TILE, TILE), F32), pltpu.VMEM((HEADS, 2 * TILE, TILE), BF16),
        SQ, SQ, SQ, pltpu.VMEM((HEADS, TILE, DH), F32),
    ]
    qh, ch, numer, raw = call(
        near_kernel, "near", 4,
        [SMEM, SMEM, natural(same), natural(same), by_head(prev), by_head(same), by_head(prev),
         by_head(same), MAPS],
        [by_head(same), by_head(same), by_head(same), part(same, 5)],
        [BIG, BIG, sds((4, HEADS, TILE, DH)), sds((4, 5, ROWS, TILE))],
        attend_scratch,
        8, FULL,
    )(index, counts, queries, cotangent, kh, kh, vh, vh, qmap)

    qh, ch, edge_now, kh_now, vh_now, maps, raw, nloc, numer, counts = hbm(
        qh, ch, edge, kh, vh, (qmap, kmap), raw, nloc, numer, counts
    )
    numer, st, dst, halo, msg = call(
        rest_kernel, "rest", 4,
        [SMEM, SMEM, by_head(first), by_head(same), HALO, by_head(first), by_head(first), MAPS,
         MAPS, part(same, 5), part(prev), MSG, ANY],
        [by_head(first), part(same, 6), part(same), PAIR, MSG],
        [sds((4, HEADS, TILE, DH)), sds((4, 6, ROWS, TILE)), PARTS, sds((2, ROWS, TILE)), MSG_T],
        [SQ, SQ, SQ, SQ, SQ, SQ, MSG_S, pltpu.VMEM((1, 5, ROWS, TILE), F32), *attend_scratch],
        5, VMEM, {12: 0},
    )(index, counts, qh, ch, edge_now, kh_now, vh_now, *maps, raw, nloc, got, numer)

    got = exchanged(msg, SEQ)

    numer, qh, ch, local = hbm(numer, qh, ch, local)
    out, gq, dn, msg = call(
        output_kernel, "output", 4,
        [by_head(same), part(same, 6), by_head(same), by_head(same), part(prev), PAIR, MSG],
        [natural(same), whole(ROWS, TILE), part(same), MSG],
        [sds((1, 4 * TILE, HEADS, DH), BF16), sds((ROWS, TILE)), PARTS, MSG_T],
        [SQ, SQ, SQ, pltpu.VMEM((8, 128), F32), MSG_S, SQ, SQ, HEAD_S, SQ],
        5,
    )(numer, st, qh, ch, local, halo, got)

    got = exchanged(msg, SEQ)

    grads = call(
        key_grad_kernel, "key_grad", 4,
        [SMEM, by_head(back), by_head(back), part(back), part(back), whole(4, ROWS, TILE),
         whole(4, ROWS, TILE), HALO, PAIR, MSG, whole(ROWS, TILE)],
        whole(2 * ROWS, TILE),
        sds((2 * ROWS, TILE)),
        [SQ, SQ, SQ, SQ, SQ, SQ],
        3,
    )(index, kh, vh, sig_k, evict, dst, dn, edge, halo, got, gq)

    spread = call(
        spread_kernel, "spread", 1, [whole(16, 16, 128)], whole(16, 16, 128), sds((16, 16, 128)),
        [], 1,
    )
    grads = exchanged(grads.reshape(16, 16, 128), ("z", "core"))
    grads = exchanged(spread(grads), ("y", "batch"))
    grads = exchanged(spread(grads), ("z", "core"))
    grad_q, grad_k = grads.reshape(2, HEADS, RANK, DH).transpose(0, 1, 3, 2)
    return out, grad_q, grad_k


def solution(mesh):
    torus = Mesh(mesh.devices.reshape(8, 4, 2, mesh.shape["batch"]), ALL)
    rows = P("batch", SEQ, None, None)
    in_specs = (rows, rows, rows, P("batch", None, None), P(), P(), rows)
    return jax.shard_map(
        body, mesh=torus, in_specs=in_specs, out_specs=(rows, P(), P()), check_vma=False
    )
```

```python
import math

import jax
import jax.numpy as jnp
from jax import lax
from jax.experimental import pallas as pl
from jax.experimental.pallas import tpu as pltpu
from jax.sharding import Mesh
from jax.sharding import PartitionSpec as P

TILE = 128
HEADS = 16
RANK = 8
DH = 128
ROWS = HEADS * RANK
SEQ = ("z", "y", "core")
ALL = ("z", "y", "core", "batch")
SHIFT = 1.5
SCALE = 1.0 / math.sqrt(DH)
SCALE_LOG2 = SCALE * math.log2(math.e)
NEG = -1e30
VMEM = 24 * 2**20
F32 = jnp.float32
BF16 = jnp.bfloat16
NN = (((1,), (0,)), ((), ()))
NT = (((1,), (1,)), ((), ()))
TN = (((0,), (0,)), ((), ()))


def dot(a, b, dims=NN):
    return lax.dot_general(a, b, dims, preferred_element_type=F32)


def halves(x):
    hi = x.astype(BF16)
    return hi, (x - hi.astype(F32)).astype(BF16)


def stacked(*parts):
    rows = []
    for x in parts:
        hi = x.astype(BF16).astype(F32)
        rows += [hi, x - hi]
    return jnp.concatenate(rows, 0).astype(BF16)


def folded(x, at=0):
    return x[at : at + RANK] + x[at + RANK : at + 2 * RANK]


def row_sums(x):
    ones = jnp.ones((8, 128), BF16)
    hi, lo = halves(x)
    return dot(ones, hi, NT) + dot(ones, lo, NT)


def softplus_sigmoid(pre):
    e = jnp.exp(-jnp.abs(pre))
    value = jnp.maximum(pre, 0.0) + jnp.log1p(e)
    inv = 1.0 / (1.0 + e)
    return value, jnp.where(pre >= 0, inv, e * inv)


def per_head_sum(x):
    x = x.reshape(HEADS, RANK, TILE)
    x = jnp.broadcast_to(jnp.sum(x, 1, keepdims=True), x.shape)
    return x.reshape(ROWS, TILE)


def of(h):
    return pl.ds(h * RANK, RANK)


def lane_sums(x):
    return jnp.broadcast_to(jnp.sum(x, 1, keepdims=True), (ROWS, TILE))


def keys_kernel(idx_ref, cnt_ref, k_ref, v_ref, kmap_ref, kh_ref, vh_ref, local_ref,
                sig_ref, evict_ref, nloc_ref, msg_ref, pre, evict, st_all, st_ev, all_acc, nacc,
                tail, ntail, feats, msg):
    n = pl.program_id(0)
    tile = last_first(n)

    @pl.when(n == 0)
    def _():
        all_acc[...] = jnp.zeros_like(all_acc)
        nacc[...] = jnp.zeros_like(nacc)

    kh_ref[0] = jnp.swapaxes(k_ref[0], 0, 1)
    vh_ref[0] = jnp.swapaxes(v_ref[0], 0, 1)
    lanes = lax.broadcasted_iota(jnp.int32, (RANK, TILE), 1)
    for h in range(HEADS):
        pre[of(h), :] = dot(kmap_ref[h], kh_ref[0, h], NT)
        count = cnt_ref[h, idx_ref[0] * 4 + tile]
        evict[of(h), :] = (lanes >= count).astype(F32)
    feat, sig = softplus_sigmoid(pre[...] - SHIFT)
    ev = feat * evict[...]
    feats[0] = feat
    feats[1] = ev
    for h in range(HEADS):
        res = dot(stacked(feats[0, of(h), :], feats[1, of(h), :]), vh_ref[0, h])
        st_all[of(h), :] = folded(res)
        st_ev[of(h), :] = folded(res, 2 * RANK)
    evict_ref[0] = evict[...]
    sig_ref[0] = sig
    local_ref[0] = all_acc[...] + st_ev[...]
    nloc_ref[0] = lane_sums(ev) + nacc[...]

    @pl.when(n == 0)
    def _():
        tail[...] = st_all[...]
        ntail[...] = lane_sums(feat)

    @pl.when(n > 0)
    def _():
        all_acc[...] += st_all[...]
        nacc[...] += lane_sums(feat)

    @pl.when(n == 3)
    def _():
        all_acc[...] += tail[...]
        row = row_sums((nacc[...] + ntail[...]) * (1.0 / 128.0))
        for s in range(64):
            msg[s, :, 0:128] = all_acc[2 * s : 2 * s + 1, :]
            msg[s, :, 128:256] = all_acc[2 * s + 1 : 2 * s + 2, :]
            msg[s, :, 256:384] = row[0:1]
        msg_ref[...] = msg[...]


def edge_kernel(k_ref, v_ref, o_ref, sems):
    last = pl.ds(3 * TILE, TILE)
    copies = [
        pltpu.make_async_copy(ref.at[0, last], o_ref.at[i], sems.at[i])
        for i, ref in enumerate((k_ref, v_ref))
    ]
    for copy in copies:
        copy.start()
    for copy in copies:
        copy.wait()


def attend_kernel(idx_ref, cnt_ref, q_ref, c_ref, ko_ref, vo_ref, edge_ref, qmap_ref, kmap_ref,
                  nloc_ref, got_ref, qh_ref, ch_ref, numer_ref, raw_ref, st_ref, dst_ref,
                  halo_kv, halo_ref, msg_ref, kp, vv, kept, norm, norm_t, cf, dst, dacc, msg, scores,
                  weights, pre, mx, den, cs):
    t = pl.program_id(0)
    index = idx_ref[0]
    before = index * 4 + t - 1
    counts = [
        jnp.where(before >= 0, cnt_ref[h, jnp.maximum(before, 0)], 0) for h in range(HEADS)
    ]
    own, other = t % 2, (t + 1) % 2

    @pl.when(t == 0)
    def _():
        dacc[...] = jnp.zeros_like(dacc)
        run, run_1, nrun = (jnp.zeros((1, 128), F32) for _ in range(3))
        for s in range(64):
            msg[s, 0:1, :] = run
            msg[s, 1:2, :] = run_1
            run = run + got_ref[s, :, 0:128]
            run_1 = run_1 + got_ref[s, :, 128:256]
            nrun = nrun + jnp.where(s < index, got_ref[s, :, 256:384], 0.0)
        norm[...] = jnp.broadcast_to(nrun, (128, 128)).T
        kp[...] = jnp.swapaxes(edge_ref[0], 0, 1)
        vv[1] = jnp.swapaxes(edge_ref[1], 0, 1)
        halo_kv[0] = kp[...]
        halo_kv[1] = vv[1]
        lanes = lax.broadcasted_iota(jnp.int32, (RANK, TILE), 1)
        for h in range(HEADS):
            pre[of(h), :] = dot(kmap_ref[h], kp[h], NT)
            kept[of(h), :] = (lanes < counts[h]).astype(F32)
        feat, sig = softplus_sigmoid(pre[...] - SHIFT)
        feat = feat * kept[...]
        cf[...] = feat
        for h in range(HEADS):
            dst[of(h), :] = folded(dot(stacked(cf[of(h), :]), vv[1, h]))
        halo_ref[0] = dst[...]
        halo_ref[1] = kept[...] * sig
        norm_t[...] = norm[...] - lane_sums(feat)

    @pl.when(t > 0)
    def _():
        norm_t[...] = norm[...] + nloc_ref[0]

    qh_ref[0] = jnp.swapaxes(q_ref[0], 0, 1)
    cs[...] = jnp.swapaxes(c_ref[0], 0, 1)
    ch_ref[0] = cs[...]
    vv[own] = vo_ref[0]
    rows = lax.broadcasted_iota(jnp.int32, (TILE, TILE), 0)
    cols = lax.broadcasted_iota(jnp.int32, (TILE, TILE), 1)
    causal = rows <= cols
    zeros = jnp.zeros((RANK, DH), F32)
    for h in range(HEADS):
        top = jnp.concatenate([qmap_ref[h].astype(F32), zeros], 0).astype(BF16)
        res = dot(jnp.concatenate([top, kp[h], ko_ref[0, h]], 0), qh_ref[0, h], NT)
        pre[of(h), :] = res[:RANK]
        s_prev = jnp.where(rows < counts[h], res[2 * RANK : 2 * RANK + TILE], NEG)
        s_own = jnp.where(causal, res[2 * RANK + TILE :], NEG)
        scores[h, 0:TILE, :] = s_prev
        scores[h, TILE:, :] = s_own
        top = jnp.max(jnp.maximum(s_prev, s_own), 0, keepdims=True)
        mx[of(h), :] = jnp.broadcast_to(top, (RANK, TILE))
    kp[...] = ko_ref[0]
    for h in range(HEADS):
        s = scores[h].reshape(2 * TILE // RANK, RANK, TILE)
        w = jnp.exp2((s - mx[of(h), :][None]) * SCALE_LOG2)
        weights[h] = w.reshape(2 * TILE, TILE).astype(BF16)
        den[of(h), :] = jnp.sum(w, 0)
    along = jnp.zeros((TILE, ROWS), F32)
    for h in range(HEADS):
        v = jnp.concatenate([vv[other, h], vv[own, h]], 0)
        numer = dot(weights[h], v, TN)
        numer_ref[0, h] = numer
        sums = jnp.sum(numer * cs[h].astype(F32), 1, keepdims=True)
        along = jnp.where(cols == h * RANK, sums, along)
    cn = along.T
    feat, sig = softplus_sigmoid(pre[...] - SHIFT)
    decay = jnp.exp(-(mx[...] * SCALE))
    rinv = 1.0 / per_head_sum(den[...] + decay * feat * norm_t[...])
    coef = decay * rinv
    cf[...] = feat * coef
    for h in range(HEADS):
        dst[of(h), :] = folded(dot(stacked(cf[of(h), :]), cs[h]))
    st_ref[0, 0] = coef
    st_ref[0, 1] = rinv
    st_ref[0, 2] = norm_t[...]
    raw_ref[0, 0] = feat
    raw_ref[0, 1] = sig
    raw_ref[0, 2] = cn
    dst_ref[0] = dst[...]
    dacc[...] += dst[...]

    @pl.when(t == 3)
    def _():
        for s in range(64):
            msg[s, 2:4, :] = dacc[2 * s : 2 * s + 2, :]
        msg_ref[...] = msg[...]


def output_kernel(numer_ref, raw_ref, st_ref, qh_ref, ch_ref, local_ref, halo_ref, got_ref,
                  out_ref, gq_ref, dn_ref, msg_ref, far, state, grad, drow, msg, cf, rinv, out,
                  gq):
    t = pl.program_id(0)

    @pl.when(t == 0)
    def _():
        drow[...] = jnp.zeros_like(drow)
        gq[...] = jnp.zeros_like(gq)
        run = jnp.zeros((2, 128), F32)
        for s in reversed(range(64)):
            far[2 * s : 2 * s + 2, :] = got_ref[s, 0:2, :]
            msg[s, :, 0:128] = run[0:1]
            msg[s, :, 128:256] = run[1:2]
            run = run + got_ref[s, 2:4, :]
        state[...] = far[...] - halo_ref[0]

    @pl.when(t > 0)
    def _():
        state[...] = far[...] + local_ref[0]

    coef = st_ref[0, 0]
    cf[...] = raw_ref[0, 0] * coef
    rinv[...] = st_ref[0, 1]
    sub = lax.broadcasted_iota(jnp.int32, (RANK, TILE), 0)
    ones = jnp.ones((RANK, DH), F32)
    zeros = jnp.zeros((RANK, DH), F32)
    for h in range(HEADS):
        s = state[of(h), :]
        s_hi = s.astype(BF16).astype(F32)
        s_lo = s - s_hi
        c = cf[of(h), :]
        c_hi = c.astype(BF16).astype(F32)
        r = rinv[of(h), :]
        r_hi = r.astype(BF16).astype(F32)
        r_mid = (r - r_hi).astype(BF16).astype(F32)
        pieces = jnp.where(sub == 0, r_hi, jnp.where(sub == 1, r_mid, r - r_hi - r_mid))
        pieces = jnp.where(sub < 3, pieces, 0.0)
        grad[of(h), :] = folded(dot(stacked(s), ch_ref[0, h], NT))
        lhs = jnp.concatenate([c_hi, c - c_hi, c_hi, pieces], 0).astype(BF16)
        left = jnp.concatenate([s_hi, s_hi, s_lo, zeros], 0)
        right = jnp.concatenate([zeros, zeros, zeros, ones], 0)
        both = dot(lhs, jnp.concatenate([left, right], 1).astype(BF16), TN)
        out[h] = (numer_ref[0, h] * both[:, DH:] + both[:, :DH]).astype(BF16)
    along = per_head_sum(raw_ref[0, 2] * rinv[...] + cf[...] * grad[...])
    dn = -(cf[...] * along)
    grad[...] = coef * (grad[...] - along * st_ref[0, 2]) * raw_ref[0, 1]
    for h in range(HEADS):
        gq[of(h), :] += folded(dot(stacked(grad[of(h), :]), qh_ref[0, h]))
    out_ref[0] = jnp.swapaxes(out[...], 0, 1)
    dn_ref[0] = lane_sums(dn)
    drow[...] += row_sums(dn)

    @pl.when(t == 3)
    def _():
        gq_ref[...] = gq[...]
        for s in range(64):
            msg[s, :, 256:384] = drow[0:1, :]
        msg_ref[...] = msg[...]


def key_grad_kernel(idx_ref, kh_ref, vh_ref, sig_ref, evict_ref, dst_ref, dn_ref, halo_in,
                    halo_ref, got_ref, gq_ref, out_ref, acc, nacc, grad, ev, near, gk):
    i = pl.program_id(0)
    n = 3 - i
    index = idx_ref[0]

    @pl.when(i == 0)
    def _():
        nrun = jnp.zeros((1, 128), F32)
        for s in range(64):
            acc[2 * s : 2 * s + 1, :] = got_ref[s, :, 0:128]
            acc[2 * s + 1 : 2 * s + 2, :] = got_ref[s, :, 128:256]
            nrun = nrun + jnp.where(s > index, got_ref[s, :, 256:384], 0.0)
        nacc[...] = jnp.broadcast_to(nrun, (128, 128)).T
        near[...] = dst_ref[0]
        for h in range(HEADS):
            grad[of(h), :] = folded(dot(stacked(near[of(h), :]), halo_in[1, h], NT))
        grad[...] = -(grad[...] + dn_ref[0]) * halo_ref[1]
        for h in range(HEADS):
            gk[of(h), :] = folded(dot(stacked(grad[of(h), :]), halo_in[0, h]))

    @pl.when(i >= 2)
    def _():
        acc[...] += dst_ref[jnp.minimum(n + 2, 3)]
        nacc[...] += dn_ref[jnp.minimum(n + 2, 3)]

    after = jnp.minimum(n + 1, 3)
    live = (n < 3).astype(F32)
    near[...] = dst_ref[after] * live
    for h in range(HEADS):
        res = dot(stacked(acc[of(h), :], near[of(h), :]), vh_ref[0, h], NT)
        grad[of(h), :] = folded(res)
        ev[of(h), :] = folded(res, 2 * RANK)
    grad[...] = (
        grad[...] + nacc[...] + evict_ref[0] * (ev[...] + dn_ref[after] * live)
    ) * sig_ref[0]
    for h in range(HEADS):
        gk[of(h), :] += folded(dot(stacked(grad[of(h), :]), kh_ref[0, h]))

    @pl.when(i == 3)
    def _():
        out_ref[:ROWS, :] = gq_ref[...]
        out_ref[ROWS:, :] = gk[...]


def spread_kernel(x_ref, o_ref):
    o_ref[...] = jnp.broadcast_to(jnp.sum(x_ref[...], 0, keepdims=True), o_ref.shape)


def sds(shape, dtype=F32):
    return jax.ShapeDtypeStruct(shape, dtype)


def whole(*shape):
    return pl.BlockSpec(shape, lambda *_: (0,) * len(shape))


def by_head(index):
    return pl.BlockSpec((1, HEADS, TILE, DH), lambda t: (index(t), 0, 0, 0))


def part(index, *lead):
    zeros = (0,) * (len(lead) + 2)
    return pl.BlockSpec((1, *lead, ROWS, TILE), lambda t: (index(t), *zeros))


def natural(index):
    return pl.BlockSpec((1, TILE, HEADS, DH), lambda t: (0, index(t), 0, 0))


def last_first(t):
    return (t + 3) % 4


def same(t):
    return t


def prev(t):
    return jnp.maximum(t - 1, 0)


def back(t):
    return 3 - t


SMEM = pl.BlockSpec(memory_space=pltpu.SMEM)
ANY = pl.BlockSpec(memory_space=pl.ANY)
MAPS = whole(HEADS, RANK, DH)
MSG = whole(64, 4, 128)
MSG_T = sds((64, 4, 128))
MSG_S = pltpu.VMEM((64, 4, 128), F32)
SHORT = whole(64, 1, 384)
SHORT_T = sds((64, 1, 384))
SHORT_S = pltpu.VMEM((64, 1, 384), F32)
HALO = whole(2, HEADS, TILE, DH)
PAIR = whole(2, ROWS, TILE)
BIG = sds((4, HEADS, TILE, DH), BF16)
PARTS = sds((4, ROWS, TILE))
SQ = pltpu.VMEM((ROWS, TILE), F32)
HEAD_S = pltpu.VMEM((HEADS, TILE, DH), BF16)


def exchanged(x, axes):
    return lax.all_to_all(x, axes, split_axis=0, concat_axis=0, tiled=True)


def call(kernel, name, grid, in_specs, out_specs, out_shape, scratch, us, flags=None):
    return pl.pallas_call(
        kernel,
        grid=(grid,),
        in_specs=in_specs,
        out_specs=out_specs,
        out_shape=out_shape,
        scratch_shapes=scratch,
        name=name,
        cost_estimate=pl.CostEstimate(
            flops=int(us * 2e8), bytes_accessed=int(us * 1e6), transcendentals=0
        ),
        compiler_params=pltpu.CompilerParams(
            dimension_semantics=("arbitrary",), vmem_limit_bytes=VMEM, flags=flags
        ),
    )


def body(queries, keys, values, keep_count, query_map, key_map, cotangent):
    count = lax.axis_size(SEQ)
    steps = [(i, i + 1) for i in range(count - 1)]
    index = lax.axis_index(SEQ).astype(jnp.int32).reshape(1)
    counts = keep_count[0]
    qmap = query_map.transpose(0, 2, 1)
    kmap = key_map.transpose(0, 2, 1)

    keys, values, kmap_now, counts_now = (
        pltpu.with_memory_space_constraint(x, pltpu.HBM) for x in (keys, values, kmap, counts)
    )
    edge = call(
        edge_kernel, "edge", 1, [ANY, ANY], whole(2, TILE, HEADS, DH),
        sds((2, TILE, HEADS, DH), BF16), [pltpu.SemaphoreType.DMA((2,))], 1,
    )(keys, values)
    edge = lax.ppermute(edge, SEQ, steps)

    kh, vh, local, sig_k, evict, nloc, msg = call(
        keys_kernel, "keys", 4,
        [SMEM, SMEM, natural(last_first), natural(last_first), MAPS],
        [by_head(last_first), by_head(last_first), part(last_first), part(last_first),
         part(last_first), part(last_first), SHORT],
        [BIG, BIG, PARTS, PARTS, PARTS, PARTS, SHORT_T],
        [SQ, SQ, SQ, SQ, SQ, SQ, SQ, SQ, pltpu.VMEM((2, ROWS, TILE), F32), SHORT_S],
        4,
    )(index, counts_now, keys, values, kmap_now)

    got = exchanged(msg, SEQ)

    qh, ch, numer, raw, st, dst, halo_kv, halo, msg = call(
        attend_kernel, "attend", 4,
        [SMEM, SMEM, natural(same), natural(same), by_head(same), by_head(same), whole(2, TILE, HEADS, DH), MAPS, MAPS,
         part(prev), SHORT],
        [by_head(same), by_head(same), by_head(same), part(same, 3), part(same, 3), part(same),
         HALO, PAIR, MSG],
        [BIG, BIG, sds((4, HEADS, TILE, DH)), sds((4, 3, ROWS, TILE)), sds((4, 3, ROWS, TILE)),
         PARTS, sds((2, HEADS, TILE, DH), BF16), sds((2, ROWS, TILE)), MSG_T],
        [HEAD_S, pltpu.VMEM((2, HEADS, TILE, DH), BF16), SQ, SQ, SQ, SQ, SQ, SQ, MSG_S,
         pltpu.VMEM((HEADS, 2 * TILE, TILE), F32), pltpu.VMEM((HEADS, 2 * TILE, TILE), BF16),
         SQ, SQ, SQ, HEAD_S],
        10,
    )(index, counts, queries, cotangent, kh, vh, edge, qmap, kmap, nloc, got)

    got = exchanged(msg, SEQ)

    out, gq, dn, msg = call(
        output_kernel, "output", 4,
        [by_head(same), part(same, 3), part(same, 3), by_head(same), by_head(same), part(prev),
         PAIR, MSG],
        [natural(same), whole(ROWS, TILE), part(same), SHORT],
        [sds((1, 4 * TILE, HEADS, DH), BF16), sds((ROWS, TILE)), PARTS, SHORT_T],
        [SQ, SQ, SQ, pltpu.VMEM((8, 128), F32), SHORT_S, SQ, SQ, HEAD_S, SQ],
        5,
    )(numer, raw, st, qh, ch, local, halo, got)

    got = exchanged(msg, SEQ)

    grads = call(
        key_grad_kernel, "key_grad", 4,
        [SMEM, by_head(back), by_head(back), part(back), part(back), whole(4, ROWS, TILE),
         whole(4, ROWS, TILE), HALO, PAIR, SHORT, whole(ROWS, TILE)],
        whole(2 * ROWS, TILE),
        sds((2 * ROWS, TILE)),
        [SQ, SQ, SQ, SQ, SQ, SQ],
        3,
    )(index, kh, vh, sig_k, evict, dst, dn, halo_kv, halo, got, gq)

    spread = call(
        spread_kernel, "spread", 1, [whole(16, 16, 128)], whole(16, 16, 128), sds((16, 16, 128)),
        [], 1,
    )
    grads = exchanged(grads.reshape(16, 16, 128), ("z", "core"))
    grads = exchanged(spread(grads), ("y", "batch"))
    grads = exchanged(spread(grads), ("z", "core"))
    grad_q, grad_k = grads.reshape(2, HEADS, RANK, DH).transpose(0, 1, 3, 2)
    return out, grad_q, grad_k


def solution(mesh):
    torus = Mesh(mesh.devices.reshape(8, 4, 2, mesh.shape["batch"]), ALL)
    rows = P("batch", SEQ, None, None)
    in_specs = (rows, rows, rows, P("batch", None, None), P(), P(), rows)
    return jax.shard_map(
        body, mesh=torus, in_specs=in_specs, out_specs=(rows, P(), P()), check_vma=False
    )
```

```python
import math

import jax
import jax.numpy as jnp
from jax import lax
from jax.experimental import pallas as pl
from jax.experimental.pallas import tpu as pltpu
from jax.sharding import Mesh
from jax.sharding import PartitionSpec as P

TILE = 128
HEADS = 16
RANK = 8
DH = 128
ROWS = HEADS * RANK
SEQ = ("z", "y", "core")
ALL = ("z", "y", "core", "batch")
SHIFT = 1.5
SCALE = 1.0 / math.sqrt(DH)
SCALE_LOG2 = SCALE * math.log2(math.e)
NEG = -1e30
VMEM = 24 * 2**20
F32 = jnp.float32
BF16 = jnp.bfloat16
NN = (((1,), (0,)), ((), ()))
NT = (((1,), (1,)), ((), ()))
TN = (((0,), (0,)), ((), ()))


def dot(a, b, dims=NN):
    return lax.dot_general(a, b, dims, preferred_element_type=F32)


def halves(x):
    hi = x.astype(BF16)
    return hi, (x - hi.astype(F32)).astype(BF16)


def stacked(*parts):
    rows = []
    for x in parts:
        hi = x.astype(BF16).astype(F32)
        rows += [hi, x - hi]
    return jnp.concatenate(rows, 0).astype(BF16)


def folded(x, at=0):
    return x[at : at + RANK] + x[at + RANK : at + 2 * RANK]


def row_sums(x):
    ones = jnp.ones((8, 128), BF16)
    hi, lo = halves(x)
    return dot(ones, hi, NT) + dot(ones, lo, NT)


def softplus_sigmoid(pre):
    e = jnp.exp(-jnp.abs(pre))
    value = jnp.maximum(pre, 0.0) + jnp.log1p(e)
    inv = 1.0 / (1.0 + e)
    return value, jnp.where(pre >= 0, inv, e * inv)


def per_head_sum(x):
    x = x.reshape(HEADS, RANK, TILE)
    x = jnp.broadcast_to(jnp.sum(x, 1, keepdims=True), x.shape)
    return x.reshape(ROWS, TILE)


def of(h):
    return pl.ds(h * RANK, RANK)


def lane_sums(x):
    return jnp.broadcast_to(jnp.sum(x, 1, keepdims=True), (ROWS, TILE))


def keys_kernel(idx_ref, cnt_ref, k_ref, v_ref, kmap_ref, kh_ref, vh_ref, local_ref,
                sig_ref, evict_ref, nloc_ref, msg_ref, pre, evict, st_all, st_ev, all_acc, nacc,
                tail, ntail, feats, msg):
    n = pl.program_id(0)
    tile = last_first(n)

    @pl.when(n == 0)
    def _():
        all_acc[...] = jnp.zeros_like(all_acc)
        nacc[...] = jnp.zeros_like(nacc)

    kh_ref[0] = jnp.swapaxes(k_ref[0], 0, 1)
    vh_ref[0] = jnp.swapaxes(v_ref[0], 0, 1)
    lanes = lax.broadcasted_iota(jnp.int32, (RANK, TILE), 1)
    for h in range(HEADS):
        pre[of(h), :] = dot(kmap_ref[h], kh_ref[0, h], NT)
        count = cnt_ref[h, idx_ref[0] * 4 + tile]
        evict[of(h), :] = (lanes >= count).astype(F32)
    feat, sig = softplus_sigmoid(pre[...] - SHIFT)
    ev = feat * evict[...]
    feats[0] = feat
    feats[1] = ev
    for h in range(HEADS):
        res = dot(stacked(feats[0, of(h), :], feats[1, of(h), :]), vh_ref[0, h])
        st_all[of(h), :] = folded(res)
        st_ev[of(h), :] = folded(res, 2 * RANK)
    evict_ref[0] = evict[...]
    sig_ref[0] = sig
    local_ref[0] = all_acc[...] + st_ev[...]
    nloc_ref[0] = lane_sums(ev) + nacc[...]

    @pl.when(n == 0)
    def _():
        tail[...] = st_all[...]
        ntail[...] = lane_sums(feat)

    @pl.when(n > 0)
    def _():
        all_acc[...] += st_all[...]
        nacc[...] += lane_sums(feat)

    @pl.when(n == 3)
    def _():
        all_acc[...] += tail[...]
        row = row_sums((nacc[...] + ntail[...]) * (1.0 / 128.0))
        for s in range(64):
            msg[s, :, 0:128] = all_acc[2 * s : 2 * s + 1, :]
            msg[s, :, 128:256] = all_acc[2 * s + 1 : 2 * s + 2, :]
            msg[s, :, 256:384] = row[0:1]
        msg_ref[...] = msg[...]


def edge_kernel(k_ref, v_ref, o_ref, sems):
    rows = TILE // 4
    copies = [
        pltpu.make_async_copy(
            ref.at[0, pl.ds(3 * TILE + j * rows, rows)],
            o_ref.at[i, pl.ds(j * rows, rows)],
            sems.at[i, j],
        )
        for i, ref in enumerate((k_ref, v_ref))
        for j in range(4)
    ]
    for copy in copies:
        copy.start()
    for copy in copies:
        copy.wait()


def attend_kernel(idx_ref, cnt_ref, q_ref, c_ref, ko_ref, vo_ref, edge_ref, qmap_ref, kmap_ref,
                  nloc_ref, got_ref, qh_ref, ch_ref, numer_ref, raw_ref, st_ref, dst_ref,
                  halo_kv, halo_ref, msg_ref, kp, vv, kept, norm, norm_t, cf, dst, dacc, msg, scores,
                  weights, pre, mx, den, cs):
    t = pl.program_id(0)
    index = idx_ref[0]
    before = index * 4 + t - 1
    counts = [
        jnp.where(before >= 0, cnt_ref[h, jnp.maximum(before, 0)], 0) for h in range(HEADS)
    ]
    own, other = t % 2, (t + 1) % 2

    @pl.when(t == 0)
    def _():
        dacc[...] = jnp.zeros_like(dacc)
        run, run_1, nrun = (jnp.zeros((1, 128), F32) for _ in range(3))
        for s in range(64):
            msg[s, 0:1, :] = run
            msg[s, 1:2, :] = run_1
            run = run + got_ref[s, :, 0:128]
            run_1 = run_1 + got_ref[s, :, 128:256]
            nrun = nrun + jnp.where(s < index, got_ref[s, :, 256:384], 0.0)
        norm[...] = jnp.broadcast_to(nrun, (128, 128)).T
        kp[...] = jnp.swapaxes(edge_ref[0], 0, 1)
        vv[1] = jnp.swapaxes(edge_ref[1], 0, 1)
        halo_kv[0] = kp[...]
        halo_kv[1] = vv[1]
        lanes = lax.broadcasted_iota(jnp.int32, (RANK, TILE), 1)
        for h in range(HEADS):
            pre[of(h), :] = dot(kmap_ref[h], kp[h], NT)
            kept[of(h), :] = (lanes < counts[h]).astype(F32)
        feat, sig = softplus_sigmoid(pre[...] - SHIFT)
        feat = feat * kept[...]
        cf[...] = feat
        for h in range(HEADS):
            dst[of(h), :] = folded(dot(stacked(cf[of(h), :]), vv[1, h]))
        halo_ref[0] = dst[...]
        halo_ref[1] = kept[...] * sig
        norm_t[...] = norm[...] - lane_sums(feat)

    @pl.when(t > 0)
    def _():
        norm_t[...] = norm[...] + nloc_ref[0]

    qh_ref[0] = jnp.swapaxes(q_ref[0], 0, 1)
    cs[...] = jnp.swapaxes(c_ref[0], 0, 1)
    ch_ref[0] = cs[...]
    vv[own] = vo_ref[0]
    rows = lax.broadcasted_iota(jnp.int32, (TILE, TILE), 0)
    cols = lax.broadcasted_iota(jnp.int32, (TILE, TILE), 1)
    causal = rows <= cols
    zeros = jnp.zeros((RANK, DH), F32)
    for h in range(HEADS):
        top = jnp.concatenate([qmap_ref[h].astype(F32), zeros], 0).astype(BF16)
        res = dot(jnp.concatenate([top, kp[h], ko_ref[0, h]], 0), qh_ref[0, h], NT)
        pre[of(h), :] = res[:RANK]
        s_prev = jnp.where(rows < counts[h], res[2 * RANK : 2 * RANK + TILE], NEG)
        s_own = jnp.where(causal, res[2 * RANK + TILE :], NEG)
        scores[h, 0:TILE, :] = s_prev
        scores[h, TILE:, :] = s_own
        top = jnp.max(jnp.maximum(s_prev, s_own), 0, keepdims=True)
        mx[of(h), :] = jnp.broadcast_to(top, (RANK, TILE))
    kp[...] = ko_ref[0]
    for h in range(HEADS):
        s = scores[h].reshape(2 * TILE // RANK, RANK, TILE)
        w = jnp.exp2((s - mx[of(h), :][None]) * SCALE_LOG2)
        weights[h] = w.reshape(2 * TILE, TILE).astype(BF16)
        den[of(h), :] = jnp.sum(w, 0)
    along = jnp.zeros((TILE, ROWS), F32)
    for h in range(HEADS):
        v = jnp.concatenate([vv[other, h], vv[own, h]], 0)
        numer = dot(weights[h], v, TN)
        numer_ref[0, h] = numer
        sums = jnp.sum(numer * cs[h].astype(F32), 1, keepdims=True)
        along = jnp.where(cols == h * RANK, sums, along)
    cn = along.T
    feat, sig = softplus_sigmoid(pre[...] - SHIFT)
    decay = jnp.exp(-(mx[...] * SCALE))
    rinv = 1.0 / per_head_sum(den[...] + decay * feat * norm_t[...])
    coef = decay * rinv
    cf[...] = feat * coef
    for h in range(HEADS):
        dst[of(h), :] = folded(dot(stacked(cf[of(h), :]), cs[h]))
    st_ref[0, 0] = coef
    st_ref[0, 1] = rinv
    st_ref[0, 2] = norm_t[...]
    raw_ref[0, 0] = feat
    raw_ref[0, 1] = sig
    raw_ref[0, 2] = cn
    dst_ref[0] = dst[...]
    dacc[...] += dst[...]

    @pl.when(t == 3)
    def _():
        for s in range(64):
            msg[s, 2:4, :] = dacc[2 * s : 2 * s + 2, :]
        msg_ref[...] = msg[...]


def output_kernel(numer_ref, raw_ref, st_ref, qh_ref, ch_ref, local_ref, halo_ref, got_ref,
                  out_ref, gq_ref, dn_ref, msg_ref, far, state, grad, drow, msg, cf, rinv, out,
                  gq):
    t = pl.program_id(0)

    @pl.when(t == 0)
    def _():
        drow[...] = jnp.zeros_like(drow)
        gq[...] = jnp.zeros_like(gq)
        run = jnp.zeros((2, 128), F32)
        for s in reversed(range(64)):
            far[2 * s : 2 * s + 2, :] = got_ref[s, 0:2, :]
            msg[s, :, 0:128] = run[0:1]
            msg[s, :, 128:256] = run[1:2]
            run = run + got_ref[s, 2:4, :]
        state[...] = far[...] - halo_ref[0]

    @pl.when(t > 0)
    def _():
        state[...] = far[...] + local_ref[0]

    coef = st_ref[0, 0]
    cf[...] = raw_ref[0, 0] * coef
    rinv[...] = st_ref[0, 1]
    sub = lax.broadcasted_iota(jnp.int32, (RANK, TILE), 0)
    ones = jnp.ones((RANK, DH), F32)
    zeros = jnp.zeros((RANK, DH), F32)
    for h in range(HEADS):
        s = state[of(h), :]
        s_hi = s.astype(BF16).astype(F32)
        s_lo = s - s_hi
        c = cf[of(h), :]
        c_hi = c.astype(BF16).astype(F32)
        r = rinv[of(h), :]
        r_hi = r.astype(BF16).astype(F32)
        r_mid = (r - r_hi).astype(BF16).astype(F32)
        pieces = jnp.where(sub == 0, r_hi, jnp.where(sub == 1, r_mid, r - r_hi - r_mid))
        pieces = jnp.where(sub < 3, pieces, 0.0)
        grad[of(h), :] = folded(dot(stacked(s), ch_ref[0, h], NT))
        lhs = jnp.concatenate([c_hi, c - c_hi, c_hi, pieces], 0).astype(BF16)
        left = jnp.concatenate([s_hi, s_hi, s_lo, zeros], 0)
        right = jnp.concatenate([zeros, zeros, zeros, ones], 0)
        both = dot(lhs, jnp.concatenate([left, right], 1).astype(BF16), TN)
        out[h] = (numer_ref[0, h] * both[:, DH:] + both[:, :DH]).astype(BF16)
    along = per_head_sum(raw_ref[0, 2] * rinv[...] + cf[...] * grad[...])
    dn = -(cf[...] * along)
    grad[...] = coef * (grad[...] - along * st_ref[0, 2]) * raw_ref[0, 1]
    for h in range(HEADS):
        gq[of(h), :] += folded(dot(stacked(grad[of(h), :]), qh_ref[0, h]))
    out_ref[0] = jnp.swapaxes(out[...], 0, 1)
    dn_ref[0] = lane_sums(dn)
    drow[...] += row_sums(dn)

    @pl.when(t == 3)
    def _():
        gq_ref[...] = gq[...]
        for s in range(64):
            msg[s, :, 256:384] = drow[0:1, :]
        msg_ref[...] = msg[...]


def key_grad_kernel(idx_ref, kh_ref, vh_ref, sig_ref, evict_ref, dst_ref, dn_ref, halo_in,
                    halo_ref, got_ref, gq_ref, out_ref, acc, nacc, grad, ev, near, gk):
    i = pl.program_id(0)
    n = 3 - i
    index = idx_ref[0]

    @pl.when(i == 0)
    def _():
        nrun = jnp.zeros((1, 128), F32)
        for s in range(64):
            acc[2 * s : 2 * s + 1, :] = got_ref[s, :, 0:128]
            acc[2 * s + 1 : 2 * s + 2, :] = got_ref[s, :, 128:256]
            nrun = nrun + jnp.where(s > index, got_ref[s, :, 256:384], 0.0)
        nacc[...] = jnp.broadcast_to(nrun, (128, 128)).T
        near[...] = dst_ref[0]
        for h in range(HEADS):
            grad[of(h), :] = folded(dot(stacked(near[of(h), :]), halo_in[1, h], NT))
        grad[...] = -(grad[...] + dn_ref[0]) * halo_ref[1]
        for h in range(HEADS):
            gk[of(h), :] = folded(dot(stacked(grad[of(h), :]), halo_in[0, h]))

    @pl.when(i >= 2)
    def _():
        acc[...] += dst_ref[jnp.minimum(n + 2, 3)]
        nacc[...] += dn_ref[jnp.minimum(n + 2, 3)]

    after = jnp.minimum(n + 1, 3)
    live = (n < 3).astype(F32)
    near[...] = dst_ref[after] * live
    for h in range(HEADS):
        res = dot(stacked(acc[of(h), :], near[of(h), :]), vh_ref[0, h], NT)
        grad[of(h), :] = folded(res)
        ev[of(h), :] = folded(res, 2 * RANK)
    grad[...] = (
        grad[...] + nacc[...] + evict_ref[0] * (ev[...] + dn_ref[after] * live)
    ) * sig_ref[0]
    for h in range(HEADS):
        gk[of(h), :] += folded(dot(stacked(grad[of(h), :]), kh_ref[0, h]))

    @pl.when(i == 3)
    def _():
        out_ref[:ROWS, :] = gq_ref[...]
        out_ref[ROWS:, :] = gk[...]


def spread_kernel(x_ref, o_ref):
    o_ref[...] = jnp.broadcast_to(jnp.sum(x_ref[...], 0, keepdims=True), o_ref.shape)


def sds(shape, dtype=F32):
    return jax.ShapeDtypeStruct(shape, dtype)


def whole(*shape):
    return pl.BlockSpec(shape, lambda *_: (0,) * len(shape))


def by_head(index):
    return pl.BlockSpec((1, HEADS, TILE, DH), lambda t: (index(t), 0, 0, 0))


def part(index, *lead):
    zeros = (0,) * (len(lead) + 2)
    return pl.BlockSpec((1, *lead, ROWS, TILE), lambda t: (index(t), *zeros))


def natural(index):
    return pl.BlockSpec((1, TILE, HEADS, DH), lambda t: (0, index(t), 0, 0))


def last_first(t):
    return (t + 3) % 4


def same(t):
    return t


def prev(t):
    return jnp.maximum(t - 1, 0)


def back(t):
    return 3 - t


SMEM = pl.BlockSpec(memory_space=pltpu.SMEM)
ANY = pl.BlockSpec(memory_space=pl.ANY)
MAPS = whole(HEADS, RANK, DH)
MSG = whole(64, 4, 128)
MSG_T = sds((64, 4, 128))
MSG_S = pltpu.VMEM((64, 4, 128), F32)
SHORT = whole(64, 1, 384)
SHORT_T = sds((64, 1, 384))
SHORT_S = pltpu.VMEM((64, 1, 384), F32)
HALO = whole(2, HEADS, TILE, DH)
PAIR = whole(2, ROWS, TILE)
BIG = sds((4, HEADS, TILE, DH), BF16)
PARTS = sds((4, ROWS, TILE))
SQ = pltpu.VMEM((ROWS, TILE), F32)
HEAD_S = pltpu.VMEM((HEADS, TILE, DH), BF16)


def exchanged(x, axes):
    return lax.all_to_all(x, axes, split_axis=0, concat_axis=0, tiled=True)


def call(kernel, name, grid, in_specs, out_specs, out_shape, scratch, us, flags=None):
    return pl.pallas_call(
        kernel,
        grid=(grid,),
        in_specs=in_specs,
        out_specs=out_specs,
        out_shape=out_shape,
        scratch_shapes=scratch,
        name=name,
        cost_estimate=pl.CostEstimate(
            flops=int(us * 2e8), bytes_accessed=int(us * 1e6), transcendentals=0
        ),
        compiler_params=pltpu.CompilerParams(
            dimension_semantics=("arbitrary",), vmem_limit_bytes=VMEM, flags=flags
        ),
    )


def body(queries, keys, values, keep_count, query_map, key_map, cotangent):
    count = lax.axis_size(SEQ)
    steps = [(i, i + 1) for i in range(count - 1)]
    index = lax.axis_index(SEQ).astype(jnp.int32).reshape(1)
    counts = keep_count[0]
    qmap = query_map.transpose(0, 2, 1)
    kmap = key_map.transpose(0, 2, 1)

    keys, values, kmap_now, counts_now, queries, cotangent = (
        pltpu.with_memory_space_constraint(x, pltpu.HBM)
        for x in (keys, values, kmap, counts, queries, cotangent)
    )
    edge = call(
        edge_kernel, "edge", 1, [ANY, ANY], whole(2, TILE, HEADS, DH),
        sds((2, TILE, HEADS, DH), BF16), [pltpu.SemaphoreType.DMA((2, 4))], 1,
    )(keys, values)
    edge = lax.ppermute(edge, SEQ, steps)

    kh, vh, local, sig_k, evict, nloc, msg = call(
        keys_kernel, "keys", 4,
        [SMEM, SMEM, natural(last_first), natural(last_first), MAPS],
        [by_head(last_first), by_head(last_first), part(last_first), part(last_first),
         part(last_first), part(last_first), SHORT],
        [BIG, BIG, PARTS, PARTS, PARTS, PARTS, SHORT_T],
        [SQ, SQ, SQ, SQ, SQ, SQ, SQ, SQ, pltpu.VMEM((2, ROWS, TILE), F32), SHORT_S],
        4,
    )(index, counts_now, keys, values, kmap_now)

    got = exchanged(msg, SEQ)

    qh, ch, numer, raw, st, dst, halo_kv, halo, msg = call(
        attend_kernel, "attend", 4,
        [SMEM, SMEM, natural(same), natural(same), by_head(same), by_head(same), whole(2, TILE, HEADS, DH), MAPS, MAPS,
         part(prev), SHORT],
        [by_head(same), by_head(same), by_head(same), part(same, 3), part(same, 3), part(same),
         HALO, PAIR, MSG],
        [BIG, BIG, sds((4, HEADS, TILE, DH)), sds((4, 3, ROWS, TILE)), sds((4, 3, ROWS, TILE)),
         PARTS, sds((2, HEADS, TILE, DH), BF16), sds((2, ROWS, TILE)), MSG_T],
        [HEAD_S, pltpu.VMEM((2, HEADS, TILE, DH), BF16), SQ, SQ, SQ, SQ, SQ, SQ, MSG_S,
         pltpu.VMEM((HEADS, 2 * TILE, TILE), F32), pltpu.VMEM((HEADS, 2 * TILE, TILE), BF16),
         SQ, SQ, SQ, HEAD_S],
        10,
    )(index, counts, queries, cotangent, kh, vh, edge, qmap, kmap, nloc, got)

    got = exchanged(msg, SEQ)

    out, gq, dn, msg = call(
        output_kernel, "output", 4,
        [by_head(same), part(same, 3), part(same, 3), by_head(same), by_head(same), part(prev),
         PAIR, MSG],
        [natural(same), whole(ROWS, TILE), part(same), SHORT],
        [sds((1, 4 * TILE, HEADS, DH), BF16), sds((ROWS, TILE)), PARTS, SHORT_T],
        [SQ, SQ, SQ, pltpu.VMEM((8, 128), F32), SHORT_S, SQ, SQ, HEAD_S, SQ],
        5,
    )(numer, raw, st, qh, ch, local, halo, got)

    got = exchanged(msg, SEQ)

    grads = call(
        key_grad_kernel, "key_grad", 4,
        [SMEM, by_head(back), by_head(back), part(back), part(back), whole(4, ROWS, TILE),
         whole(4, ROWS, TILE), HALO, PAIR, SHORT, whole(ROWS, TILE)],
        whole(2 * ROWS, TILE),
        sds((2 * ROWS, TILE)),
        [SQ, SQ, SQ, SQ, SQ, SQ],
        3,
    )(index, kh, vh, sig_k, evict, dst, dn, halo_kv, halo, got, gq)

    spread = call(
        spread_kernel, "spread", 1, [whole(16, 16, 128)], whole(16, 16, 128), sds((16, 16, 128)),
        [], 1,
    )
    grads = exchanged(grads.reshape(16, 16, 128), ("y", "batch"))
    grads = exchanged(spread(grads), ("z", "core"))
    grads = exchanged(spread(grads), ("y", "batch"))
    grad_q, grad_k = grads.reshape(2, HEADS, RANK, DH).transpose(0, 1, 3, 2)
    return out, grad_q, grad_k


def solution(mesh):
    torus = Mesh(mesh.devices.reshape(8, 4, 2, mesh.shape["batch"]), ALL)
    rows = P("batch", SEQ, None, None)
    in_specs = (rows, rows, rows, P("batch", None, None), P(), P(), rows)
    return jax.shard_map(
        body, mesh=torus, in_specs=in_specs, out_specs=(rows, P(), P()), check_vma=False
    )
```
